128 devices in a mesh: dp: 1, ep: 128 (over z, y, x, core).
Axes of the slice: x: 4, y: 4, z: 4, core: 2. Of those that a mesh axis runs over, the one named last changes fastest.
Arguments:
- tokens_a: bfloat16 [16384, 2048], P(('dp', 'ep'))
- experts_a: int32 [16384, 8], P(('dp', 'ep'))
- slots_a: int32 [16384, 8], P(('dp', 'ep'))
- gates_a: bfloat16 [16384, 8], P(('dp', 'ep'))
- tokens_b: bfloat16 [16384, 2048], P(('dp', 'ep'))
- experts_b: int32 [16384, 8], P(('dp', 'ep'))
- slots_b: int32 [16384, 8], P(('dp', 'ep'))
- gates_b: bfloat16 [16384, 8], P(('dp', 'ep'))
- attn_gain: bfloat16 [2048], replicated
- w_query: bfloat16 [2048, 32, 64], replicated
- w_key: bfloat16 [2048, 32, 64], replicated
- w_value: bfloat16 [2048, 32, 64], replicated
- w_out: bfloat16 [32, 64, 2048], replicated
- moe_gain: bfloat16 [2048], replicated
- w_gate: bfloat16 [128, 2048, 768], P('ep')
- w_up: bfloat16 [128, 2048, 768], P('ep')
- w_down: bfloat16 [128, 768, 2048], P('ep')
Outputs:
- output 1: bfloat16 [16384, 2048], P(('dp', 'ep'))
- output 2: bfloat16 [16384, 2048], P(('dp', 'ep'))
All inputs are finite; a program needn't handle non-finite values.
Results may differ from the reference program's by a relative error of at most 0.0156055.
Values are sent between devices in bfloat16 or wider.
A program may use at most 1 GiB of HBM per device.

```python
import jax
import jax.numpy as jnp
from jax import lax

MODEL_DIM = 2048
FFN_DIM = 768
EXPERTS = 128
TOP_K = 8
HEADS = 32
TOKENS = 128
GROUP = 128
SLOTS = 16

HEAD_DIM = MODEL_DIM // HEADS
ROWS = GROUP * TOKENS
NORM_EPS = 1e-6
MASK_VALUE = -1e30


def draw_routing(route_key):
    key_start, key_hot, key_pick = jax.random.split(route_key, 3)
    spacing = EXPERTS // TOP_K
    hot_span = max(1, EXPERTS // (4 * TOP_K))
    start_any = jax.random.randint(key_start, (ROWS,), 0, EXPERTS)
    start_hot = jax.random.randint(key_hot, (ROWS,), 0, hot_span)
    use_hot = jax.random.randint(key_pick, (ROWS,), 0, 2) == 1
    position = jnp.arange(ROWS) % TOKENS
    first_expert = jnp.where(use_hot, start_hot, start_any)
    first_expert = jnp.where(position <= SLOTS, 0, first_expert)
    choice = (first_expert[:, None] + spacing * jnp.arange(TOP_K)[None, :]) % EXPERTS
    choice = choice.astype(jnp.int32)

    def device_slots(dev_choice):
        flat_ids = dev_choice.reshape(-1)
        onehot = (flat_ids[:, None] == jnp.arange(EXPERTS)[None, :]).astype(jnp.int32)
        rank_pos = jnp.sum(jnp.cumsum(onehot, axis=0) * onehot, axis=1) - 1
        return jnp.where(rank_pos < SLOTS, rank_pos, -1).reshape(TOKENS, TOP_K)

    slot_ids = lax.map(device_slots, choice.reshape(GROUP, TOKENS, TOP_K))
    return choice, slot_ids.reshape(ROWS, TOP_K).astype(jnp.int32)


def setup_inputs(seed: int = 0, part: int = 0) -> dict:
    base_key = jax.random.key(seed)
    part_key = jax.random.fold_in(base_key, part)
    part_keys = jax.random.split(part_key, 6)
    shared_keys = jax.random.split(base_key, 9)
    scale_in = MODEL_DIM ** -0.5
    scale_ffn = FFN_DIM ** -0.5
    experts_a, slots_a = draw_routing(part_keys[1])
    experts_b, slots_b = draw_routing(part_keys[4])
    return {
        "tokens_a": jax.random.normal(part_keys[0], (ROWS, MODEL_DIM), jnp.float32).astype(jnp.bfloat16),
        "experts_a": experts_a,
        "slots_a": slots_a,
        "gates_a": jax.random.uniform(part_keys[2], (ROWS, TOP_K), jnp.float32, 0.5, 1.5).astype(jnp.bfloat16),
        "tokens_b": jax.random.normal(part_keys[3], (ROWS, MODEL_DIM), jnp.float32).astype(jnp.bfloat16),
        "experts_b": experts_b,
        "slots_b": slots_b,
        "gates_b": jax.random.uniform(part_keys[5], (ROWS, TOP_K), jnp.float32, 0.5, 1.5).astype(jnp.bfloat16),
        "attn_gain": (1.0 + 0.3 * jax.random.normal(shared_keys[0], (MODEL_DIM,), jnp.float32)).astype(jnp.bfloat16),
        "w_query": (1.5 * scale_in * jax.random.normal(shared_keys[1], (MODEL_DIM, HEADS, HEAD_DIM), jnp.float32)).astype(jnp.bfloat16),
        "w_key": (1.5 * scale_in * jax.random.normal(shared_keys[2], (MODEL_DIM, HEADS, HEAD_DIM), jnp.float32)).astype(jnp.bfloat16),
        "w_value": (scale_in * jax.random.normal(shared_keys[3], (MODEL_DIM, HEADS, HEAD_DIM), jnp.float32)).astype(jnp.bfloat16),
        "w_out": (scale_in * jax.random.normal(shared_keys[4], (HEADS, HEAD_DIM, MODEL_DIM), jnp.float32)).astype(jnp.bfloat16),
        "moe_gain": (1.0 + 0.3 * jax.random.normal(shared_keys[5], (MODEL_DIM,), jnp.float32)).astype(jnp.bfloat16),
        "w_gate": (scale_in * jax.random.normal(shared_keys[6], (EXPERTS, MODEL_DIM, FFN_DIM), jnp.float32)).astype(jnp.bfloat16),
        "w_up": (scale_in * jax.random.normal(shared_keys[7], (EXPERTS, MODEL_DIM, FFN_DIM), jnp.float32)).astype(jnp.bfloat16),
        "w_down": (scale_ffn * jax.random.normal(shared_keys[8], (EXPERTS, FFN_DIM, MODEL_DIM), jnp.float32)).astype(jnp.bfloat16),
    }


def rms_norm(rows, gain_vec):
    rows_f = rows.astype(jnp.float32)
    inv_rms = lax.rsqrt(jnp.mean(rows_f * rows_f, axis=-1, keepdims=True) + NORM_EPS)
    return (rows_f * inv_rms * gain_vec.astype(jnp.float32)).astype(jnp.bfloat16)


def attention_block(sequence, attn_gain, w_query, w_key, w_value, w_out):
    normed = rms_norm(sequence, attn_gain).astype(jnp.float32)
    query = jnp.einsum("td,dhe->the", normed, w_query.astype(jnp.float32)).astype(jnp.bfloat16)
    keys = jnp.einsum("td,dhe->the", normed, w_key.astype(jnp.float32)).astype(jnp.bfloat16)
    values = jnp.einsum("td,dhe->the", normed, w_value.astype(jnp.float32)).astype(jnp.bfloat16)
    scores = jnp.einsum("qhe,khe->hqk", query.astype(jnp.float32), keys.astype(jnp.float32)) * (HEAD_DIM ** -0.5)
    causal = jnp.arange(TOKENS)[:, None] >= jnp.arange(TOKENS)[None, :]
    scores = jnp.where(causal[None, :, :], scores, MASK_VALUE)
    attn_prob = jax.nn.softmax(scores, axis=-1).astype(jnp.bfloat16)
    context = jnp.einsum("hqk,khe->qhe", attn_prob.astype(jnp.float32), values.astype(jnp.float32)).astype(jnp.bfloat16)
    attn_out = jnp.einsum("qhe,hed->qd", context.astype(jnp.float32), w_out.astype(jnp.float32))
    return (sequence.astype(jnp.float32) + attn_out).astype(jnp.bfloat16)


def moe_layer(tokens, experts, slots, gates, attn_gain, w_query, w_key, w_value, w_out, moe_gain, w_gate, w_up, w_down):
    residual = lax.map(lambda sequence: attention_block(sequence, attn_gain, w_query, w_key, w_value, w_out), tokens.reshape(GROUP, TOKENS, MODEL_DIM))
    normed = rms_norm(residual, moe_gain).reshape(ROWS, MODEL_DIM)
    row_ids = jnp.arange(ROWS, dtype=jnp.int32)
    owner = row_ids // TOKENS
    buffer_rows = EXPERTS * GROUP * SLOTS
    dest_row = jnp.where(slots >= 0, experts * (GROUP * SLOTS) + owner[:, None] * SLOTS + slots, buffer_rows)
    token_of = jnp.broadcast_to(row_ids[:, None], (ROWS, TOP_K)).reshape(-1)
    source = jnp.full((buffer_rows,), ROWS, jnp.int32).at[dest_row.reshape(-1)].set(token_of, mode="drop")

    def expert_ffn(operands):
        expert_source, gate_w, up_w, down_w = operands
        rows_in = jnp.take(normed, expert_source, axis=0, mode="fill", fill_value=0)
        gate_act = jnp.dot(rows_in, gate_w, preferred_element_type=jnp.float32)
        up_act = jnp.dot(rows_in, up_w, preferred_element_type=jnp.float32)
        hidden = (jax.nn.silu(gate_act) * up_act).astype(jnp.bfloat16)
        return jnp.dot(hidden, down_w, preferred_element_type=jnp.float32).astype(jnp.bfloat16)

    expert_out = lax.map(expert_ffn, (source.reshape(EXPERTS, GROUP * SLOTS), w_gate, w_up, w_down)).reshape(buffer_rows, MODEL_DIM)

    def combine(operands):
        dev_resid, dev_dest, dev_gates = operands
        picked = jnp.take(expert_out, dev_dest, axis=0, mode="fill", fill_value=0).reshape(TOKENS, TOP_K, MODEL_DIM)
        mixed_sum = jnp.einsum("tk,tkd->td", dev_gates.astype(jnp.float32), picked.astype(jnp.float32))
        return (dev_resid.astype(jnp.float32) + mixed_sum).astype(jnp.bfloat16)

    mixed_rows = lax.map(combine, (residual, dest_row.reshape(GROUP, TOKENS * TOP_K), gates.reshape(GROUP, TOKENS, TOP_K)))
    return mixed_rows.reshape(ROWS, MODEL_DIM)


def reference(tokens_a, experts_a, slots_a, gates_a, tokens_b, experts_b, slots_b, gates_b, attn_gain, w_query, w_key, w_value, w_out, moe_gain, w_gate, w_up, w_down):
    out_a = moe_layer(tokens_a, experts_a, slots_a, gates_a, attn_gain, w_query, w_key, w_value, w_out, moe_gain, w_gate, w_up, w_down)
    out_b = moe_layer(tokens_b, experts_b, slots_b, gates_b, attn_gain, w_query, w_key, w_value, w_out, moe_gain, w_gate, w_up, w_down)
    return (out_a, out_b)
```

```python
import functools

import jax
import jax.numpy as jnp
from jax import lax
from jax.experimental import pallas as pl
from jax.experimental.pallas import tpu as pltpu
from jax.sharding import PartitionSpec as P

NORM_EPS = 1e-6
MASK_VALUE = -1e30
RING = 4
CORES = 2
SLOTS = 16
PARTS = (
    (0, 640, ("z", "y", "x")),
    (640, 640, ("x", "z", "y")),
    (1280, 768, ("y", "x", "z")),
)
STRIDE = {"z": 32, "y": 8, "x": 2}


def coords(index):
    return {"z": index // 32, "y": (index // 8) % RING, "x": (index // 2) % RING}, index % CORES


def shift_pairs(dim, delta, flip):
    pairs = []
    for index in range(RING**3 * CORES):
        pos, core = coords(index)
        pos[dim] = (pos[dim] + delta) % RING
        target = pos["z"] * 32 + pos["y"] * 8 + pos["x"] * 2 + (core ^ flip)
        pairs.append((index, target))
    return pairs


def shift(rows, dim, delta, flip=0):
    delta = delta % RING
    if delta == 0 and flip == 0:
        return rows
    return lax.ppermute(rows, "ep", shift_pairs(dim, delta, flip))


def rms_norm(rows, gain_vec):
    rows_f = rows.astype(jnp.float32)
    inv_rms = lax.rsqrt(jnp.mean(rows_f * rows_f, axis=-1, keepdims=True) + NORM_EPS)
    return (rows_f * inv_rms * gain_vec.astype(jnp.float32)).astype(jnp.bfloat16)


def attention_block(sequence, attn_gain, w_query, w_key, w_value, w_out):
    seq_len = sequence.shape[0]
    normed = rms_norm(sequence, attn_gain)
    query = jnp.einsum("td,dhe->the", normed, w_query, preferred_element_type=jnp.float32).astype(jnp.bfloat16)
    keys = jnp.einsum("td,dhe->the", normed, w_key, preferred_element_type=jnp.float32).astype(jnp.bfloat16)
    values = jnp.einsum("td,dhe->the", normed, w_value, preferred_element_type=jnp.float32).astype(jnp.bfloat16)
    scores = jnp.einsum("qhe,khe->hqk", query, keys, preferred_element_type=jnp.float32) * (w_query.shape[2] ** -0.5)
    causal = lax.broadcasted_iota(jnp.int32, (seq_len, seq_len), 0) >= lax.broadcasted_iota(jnp.int32, (seq_len, seq_len), 1)
    scores = jnp.where(causal[None, :, :], scores, MASK_VALUE)
    attn_prob = jax.nn.softmax(scores, axis=-1).astype(jnp.bfloat16)
    context = jnp.einsum("hqk,khe->qhe", attn_prob, values, preferred_element_type=jnp.float32).astype(jnp.bfloat16)
    attn_out = jnp.einsum("qhe,hed->qd", context, w_out, preferred_element_type=jnp.float32)
    return (sequence.astype(jnp.float32) + attn_out).astype(jnp.bfloat16)


def row_ids(order):
    s1, s2, s3 = order
    pos, core = coords(lax.axis_index("ep"))
    row = jnp.arange(RING * RING * CORES * SLOTS, dtype=jnp.int32)
    slot = row % SLOTS
    flip = (row // SLOTS) % CORES
    off3 = (row // (SLOTS * CORES)) % RING
    off2 = row // (SLOTS * CORES * RING)
    line = {s1: pos[s1], s2: (pos[s2] + off2) % RING, s3: (pos[s3] + off3) % RING}
    expert = line["z"] * 32 + line["y"] * 8 + line["x"] * 2 + jnp.where(flip == 1, 1 - core, core)
    ids = (expert * SLOTS + slot).astype(jnp.float32)
    return jnp.broadcast_to(ids[:, None], (ids.shape[0], 128))


def choice_ids(meta):
    expert = meta[:, 0:128].astype(jnp.float32)
    slot = meta[:, 128:256].astype(jnp.float32)
    return jnp.where(slot >= 0, expert * SLOTS + slot, -1.0)


def select_kernel(tokens, ids_ref, *refs):
    gathered, outs = refs[:RING], refs[RING:]
    ids = ids_ref[...]
    for off2, block in enumerate(gathered):
        for off1 in range(RING):
            dest = choice_ids(block[off1, tokens : tokens + 8, :])
            hit = ids == dest[0:1, :]
            for j in range(1, 8):
                hit = jnp.logical_or(hit, ids == dest[j : j + 1, :])
            onehot = jnp.where(hit, 1.0, 0.0).astype(jnp.bfloat16)
            rows = jnp.dot(onehot, block[off1, 0:tokens, :], preferred_element_type=jnp.float32).astype(jnp.bfloat16)
            for i, out in enumerate(outs):
                out[off2, off1] = rows[i * SLOTS : (i + 1) * SLOTS, :]


def select_rows(ids, gathered):
    tokens, width = gathered[0].shape[1] - 8, gathered[0].shape[2]
    out = jax.ShapeDtypeStruct((RING, RING, SLOTS, width), jnp.bfloat16)
    flops = 2 * 16 * 128 * tokens * width
    return pl.pallas_call(
        functools.partial(select_kernel, tokens),
        out_shape=(out,) * 8,
        cost_estimate=pl.CostEstimate(flops=flops * 4, bytes_accessed=2 * 16 * 256 * width * 2, transcendentals=0),
        name="select_rows",
    )(ids, *gathered)


def piece_copies(off3x, flip, pieces, block, sem, outward):
    copies = []

    def add(piece, view):
        src, dst = (view, piece) if outward else (piece, view)
        copies.append(pltpu.make_async_copy(src, dst, sem))

    start0, width0, _ = PARTS[0]
    add(pieces[0][off3x * 2 + flip], block.at[:, :, :, start0 : start0 + width0])
    start1, width1, _ = PARTS[1]
    for offy in range(RING):
        add(pieces[1][offy * 2 + flip].at[:, off3x], block.at[offy, :, :, start1 : start1 + width1])
    start2, width2, _ = PARTS[2]
    for offz in range(RING):
        add(pieces[2][offz * 2 + flip].at[off3x], block.at[:, offz, :, start2 : start2 + width2])
    return copies


def ffn_kernel(*refs):
    w_gate, w_up, w_down = refs[0:3]
    pieces = [refs[3 + 8 * k : 11 + 8 * k] for k in range(3)]
    outs = [refs[27 + 8 * k : 35 + 8 * k] for k in range(3)]
    x_v, o_v, wg_v, wu_v, wd_v, in_sem, out_sem, w_sem = refs[51:]
    blocks = RING * CORES
    weight_copies = [
        pltpu.make_async_copy(src, dst, w_sem.at[i])
        for i, (src, dst) in enumerate(((w_gate, wg_v), (w_up, wu_v), (w_down, wd_v)))
    ]
    for copy in piece_copies(0, 0, pieces, x_v.at[0], in_sem.at[0], False):
        copy.start()
    for copy in weight_copies:
        copy.start()
    for b in range(1, blocks):
        for copy in piece_copies(b // 2, b % 2, pieces, x_v.at[b], in_sem.at[b], False):
            copy.start()

    model, ffn = wg_v.shape
    rows = RING * RING * SLOTS

    def step(b, carry):
        pltpu.make_async_copy(x_v.at[b], x_v.at[b], in_sem.at[b]).wait()

        @pl.when(b == 0)
        def _():
            weight_copies[0].wait()
            weight_copies[1].wait()

        x = x_v[b].reshape(rows, model)
        gate_act = jnp.dot(x, wg_v[...], preferred_element_type=jnp.float32)
        up_act = jnp.dot(x, wu_v[...], preferred_element_type=jnp.float32)
        hidden = (jax.nn.silu(gate_act) * up_act).astype(jnp.bfloat16)

        @pl.when(b == 0)
        def _():
            weight_copies[2].wait()

        out = jnp.dot(hidden, wd_v[...], preferred_element_type=jnp.float32).astype(jnp.bfloat16)
        o_v[b] = out.reshape(RING, RING, SLOTS, model)
        for i in range(blocks):

            @pl.when(b == i)
            def _():
                for copy in piece_copies(i // 2, i % 2, outs, o_v.at[i], out_sem.at[i], True):
                    copy.start()

        return carry

    lax.fori_loop(0, blocks, step, 0)
    for b in range(blocks):
        pltpu.make_async_copy(o_v.at[b], o_v.at[b], out_sem.at[b]).wait()


def expert_ffn(pieces, w_gate, w_up, w_down):
    model, ffn = w_gate.shape
    flat = [piece for part in pieces for piece in part]
    blocks = RING * CORES
    block_shape = (blocks, RING, RING, SLOTS, model)
    outs = pl.pallas_call(
        ffn_kernel,
        out_shape=tuple(jax.ShapeDtypeStruct(piece.shape, piece.dtype) for piece in flat),
        in_specs=[pl.BlockSpec(memory_space=pl.ANY)] * (3 + len(flat)),
        out_specs=(pl.BlockSpec(memory_space=pl.ANY),) * len(flat),
        scratch_shapes=[
            pltpu.VMEM(block_shape, jnp.bfloat16),
            pltpu.VMEM(block_shape, jnp.bfloat16),
            pltpu.VMEM((model, ffn), jnp.bfloat16),
            pltpu.VMEM((model, ffn), jnp.bfloat16),
            pltpu.VMEM((ffn, model), jnp.bfloat16),
            pltpu.SemaphoreType.DMA((blocks,)),
            pltpu.SemaphoreType.DMA((blocks,)),
            pltpu.SemaphoreType.DMA((3,)),
        ],
        compiler_params=pltpu.CompilerParams(vmem_limit_bytes=44 * 1024 * 1024),
        cost_estimate=pl.CostEstimate(flops=6 * 2048 * model * ffn, bytes_accessed=26 * 1024 * 1024, transcendentals=2048 * ffn),
        name="expert_ffn",
    )(w_gate, w_up, w_down, *flat)
    return [list(outs[8 * k : 8 * k + 8]) for k in range(3)]


def combine_kernel(tokens, ids_ref, meta_ref, *refs):
    rows, outs = refs[:RING], refs[RING:]
    width = outs[0].shape[1]
    for off1 in range(RING):
        dest = choice_ids(meta_ref[off1])
        gates = meta_ref[off1, :, 256:384].astype(jnp.float32)
        total = None
        for off2 in range(RING):
            ids = ids_ref[off2 * 128 : (off2 + 1) * 128, :]
            weight = jnp.zeros((128, 128), jnp.float32)
            for j in range(8):
                weight = jnp.where(ids == dest[j : j + 1, :], gates[j : j + 1, :], weight)
            block = rows[off2][:, off1].reshape(128, width)
            part = lax.dot_general(weight.astype(jnp.bfloat16), block, (((0,), (0,)), ((), ())), preferred_element_type=jnp.float32)
            total = part if total is None else total + part
        outs[off1][...] = total


def combine_rows(ids, meta, rows, tokens):
    width = rows[0].shape[-1]
    out = jax.ShapeDtypeStruct((tokens, width), jnp.float32)
    flops = 2 * 4 * 512 * tokens * width
    return pl.pallas_call(
        functools.partial(combine_kernel, tokens),
        out_shape=(out,) * RING,
        cost_estimate=pl.CostEstimate(flops=flops * 4, bytes_accessed=8 * 512 * width, transcendentals=0),
        name="combine_rows",
    )(ids, meta, *rows)


def dispatch(normed, meta, ids):
    pieces, metas = [], []
    tokens = normed.shape[0]
    for (start, width, (s1, s2, s3)), part_ids in zip(PARTS, ids):
        own = jnp.concatenate([normed[:, start : start + width], jnp.pad(meta, ((0, 0), (0, width - meta.shape[1])))], axis=0)
        line = jnp.stack([shift(own, s1, off) for off in range(RING)])
        plane = [shift(line, s2, off) for off in range(RING)]
        chosen = select_rows(part_ids[:128], plane)
        pieces.append([shift(chosen[off * 2 + flip], s3, off, flip) for off in range(RING) for flip in range(CORES)])
        metas.append(line[:, tokens : tokens + 8, :384])
    return pieces, metas


def bring_back(outs, metas, ids, residual):
    tokens = residual.shape[0]
    columns = []
    for (start, width, (s1, s2, s3)), part_ids, meta, part in zip(PARTS, ids, metas, outs):
        back = [shift(part[off * 2 + flip], s3, -off, flip) for off in range(RING) for flip in range(CORES)]
        rows = [shift(jnp.stack([piece[off] for piece in back]), s2, -off) for off in range(RING)]
        sums = combine_rows(part_ids, meta, rows, tokens)
        total = residual[:, start : start + width].astype(jnp.float32)
        for off in range(RING):
            total = total + shift(sums[off], s1, -off)
        columns.append(total.astype(jnp.bfloat16))
    return jnp.concatenate(columns, axis=1)


def routing_rows(experts, slots, gates):
    return jnp.concatenate([experts.T.astype(jnp.bfloat16), slots.T.astype(jnp.bfloat16), gates.T], axis=1)


def solution(mesh):
    row_spec = P(("dp", "ep"), None)
    full_spec = P(None, None, None)
    gain_spec = P(None)
    expert_spec = P("ep", None, None)
    in_specs = (row_spec,) * 8 + (gain_spec,) + (full_spec,) * 4 + (gain_spec,) + (expert_spec,) * 3

    def device_fn(tokens_a, experts_a, slots_a, gates_a, tokens_b, experts_b, slots_b, gates_b, attn_gain, w_query, w_key, w_value, w_out, moe_gain, w_gate, w_up, w_down):
        w_gate, w_up, w_down = w_gate[0], w_up[0], w_down[0]
        ids = [row_ids(order) for _, _, order in PARTS]

        def front(tokens, experts, slots, gates):
            residual = attention_block(tokens, attn_gain, w_query, w_key, w_value, w_out)
            normed = rms_norm(residual, moe_gain)
            pieces, metas = dispatch(normed, routing_rows(experts, slots, gates), ids)
            return residual, pieces, metas

        res_a, pieces_a, metas_a = front(tokens_a, experts_a, slots_a, gates_a)
        res_b, pieces_b, metas_b = front(tokens_b, experts_b, slots_b, gates_b)
        out_a = bring_back(expert_ffn(pieces_a, w_gate, w_up, w_down), metas_a, ids, res_a)
        out_b = bring_back(expert_ffn(pieces_b, w_gate, w_up, w_down), metas_b, ids, res_b)
        return out_a, out_b

    return jax.shard_map(device_fn, mesh=mesh, in_specs=in_specs, out_specs=(row_spec, row_spec), check_vma=False)
```

```python
import jax
import jax.numpy as jnp
from jax import lax
from jax.experimental import pallas as pl
from jax.experimental.pallas import tpu as pltpu
from jax.sharding import PartitionSpec as P

NORM_EPS = 1e-6
MASK_VALUE = -1e30
RING = 4
CORES = 2
SLOTS = 16
PARTS = (
    (0, 640, ("z", "y", "x")),
    (640, 640, ("x", "z", "y")),
    (1280, 768, ("y", "x", "z")),
)
STRIDE = {"z": 32, "y": 8, "x": 2}

def coords(index):
    return {"z": index // 32, "y": (index // 8) % RING, "x": (index // 2) % RING}, index % CORES


def rms_norm(rows, gain_vec):
    rows_f = rows.astype(jnp.float32)
    inv_rms = lax.rsqrt(jnp.mean(rows_f * rows_f, axis=-1, keepdims=True) + NORM_EPS)
    return (rows_f * inv_rms * gain_vec.astype(jnp.float32)).astype(jnp.bfloat16)


def attention_block(sequence, attn_gain, w_query, w_key, w_value, w_out):
    seq_len = sequence.shape[0]
    normed = rms_norm(sequence, attn_gain)
    query = jnp.einsum("td,dhe->the", normed, w_query, preferred_element_type=jnp.float32).astype(jnp.bfloat16)
    keys = jnp.einsum("td,dhe->the", normed, w_key, preferred_element_type=jnp.float32).astype(jnp.bfloat16)
    values = jnp.einsum("td,dhe->the", normed, w_value, preferred_element_type=jnp.float32).astype(jnp.bfloat16)
    scores = jnp.einsum("qhe,khe->hqk", query, keys, preferred_element_type=jnp.float32) * (w_query.shape[2] ** -0.5)
    causal = lax.broadcasted_iota(jnp.int32, (seq_len, seq_len), 0) >= lax.broadcasted_iota(jnp.int32, (seq_len, seq_len), 1)
    scores = jnp.where(causal[None, :, :], scores, MASK_VALUE)
    attn_prob = jax.nn.softmax(scores, axis=-1).astype(jnp.bfloat16)
    context = jnp.einsum("hqk,khe->qhe", attn_prob, values, preferred_element_type=jnp.float32).astype(jnp.bfloat16)
    attn_out = jnp.einsum("qhe,hed->qd", context, w_out, preferred_element_type=jnp.float32)
    return (sequence.astype(jnp.float32) + attn_out).astype(jnp.bfloat16)


def row_ids(order):
    s1, s2, s3 = order
    pos, core = coords(lax.axis_index("ep"))
    row = jnp.arange(RING * RING * CORES * SLOTS, dtype=jnp.int32)
    slot = row % SLOTS
    flip = (row // SLOTS) % CORES
    off3 = (row // (SLOTS * CORES)) % RING
    off2 = row // (SLOTS * CORES * RING)
    line = {s1: pos[s1], s2: (pos[s2] + off2) % RING, s3: (pos[s3] + off3) % RING}
    expert = line["z"] * 32 + line["y"] * 8 + line["x"] * 2 + jnp.where(flip == 1, 1 - core, core)
    ids = (expert * SLOTS + slot).astype(jnp.float32)
    return jnp.broadcast_to(ids[:, None], (ids.shape[0], 128))


def peer(dim, delta, flip=0):
    me = lax.axis_index("ep")
    stride = STRIDE[dim]
    place = lax.rem(me // stride, RING)
    other = me + (lax.rem(place + delta % RING, RING) - place) * stride
    if flip:
        other = other + 1 - 2 * lax.rem(me, CORES)
    return {"ep": other}


def send(src, dst, send_sem, recv_sem, where):
    return pltpu.make_async_remote_copy(src_ref=src, dst_ref=dst, send_sem=send_sem, recv_sem=recv_sem, device_id=where, device_id_type=pl.DeviceIdType.MESH)


def drain(ref, sem):
    pltpu.make_async_copy(ref, ref, sem).wait()


def enter():
    barrier = pltpu.get_barrier_semaphore()
    count = 0
    for dim in ("x", "y", "z"):
        for delta in range(1, RING):
            for flip in range(CORES):
                pl.semaphore_signal(barrier, inc=1, device_id=peer(dim, delta, flip), device_id_type=pl.DeviceIdType.MESH)
                count += 1
    pl.semaphore_signal(barrier, inc=1, device_id=peer("x", 0, 1), device_id_type=pl.DeviceIdType.MESH)
    pl.semaphore_wait(barrier, count + 1)


def group_view(rows, part, off3, flip, off2):
    start, width, (_, s2, s3) = PARTS[part]
    place = {s3: off3, s2: off2}
    index = tuple(place.get(dim, slice(None)) for dim in ("y", "z"))
    line = flip * RING + place["x"] if "x" in place else slice(flip * RING, (flip + 1) * RING)
    return rows.at[line, index[0], index[1], :, start : start + width]


PAIRS = tuple((off, flip) for off in range(RING) for flip in range(CORES))


def routing_ids(meta):
    expert = meta[:, 0:128].astype(jnp.float32)
    slot = meta[:, 128:256].astype(jnp.float32)
    return jnp.where(slot >= 0, expert * SLOTS + slot, -1.0)


def dispatch_kernel(ids_ref, *refs):
    batches = 2
    own_refs, out_refs, meta_refs = refs[0:2], refs[2:4], refs[4:6]
    planes = [refs[6 + 3 * n : 9 + 3 * n] for n in range(batches)]
    chosen = [refs[12 + 3 * n : 15 + 3 * n] for n in range(batches)]
    plane_recv, plane_send, row_recv, row_send, local_sem = refs[18:]
    tokens = own_refs[0].shape[0] - 8
    enter()

    def own_part(n, part):
        start, width, _ = PARTS[part]
        return own_refs[n].at[:, start : start + width]

    for n in range(batches):
        for part, (_, _, (s1, s2, _)) in enumerate(PARTS):
            plane = planes[n][part]
            for off in (1, 3, 2):
                send(own_part(n, part), plane.at[off], plane_send.at[n, part], plane_recv.at[n, part, off], peer(s1, off)).start()
                send(own_part(n, part), plane.at[off * RING], plane_send.at[n, part], plane_recv.at[n, part, off * RING], peer(s2, off)).start()

    def forward(n):
        for part, (_, _, (s1, s2, _)) in enumerate(PARTS):
            plane = planes[n][part]
            for off1 in (1, 3, 2):
                drain(plane.at[off1], plane_recv.at[n, part, off1])
                for off2 in (1, 3, 2):
                    send(plane.at[off1], plane.at[off2 * RING + off1], plane_send.at[n, part], plane_recv.at[n, part, off2 * RING + off1], peer(s2, off2)).start()

    def select(n, part, off2, off1, block):
        width = PARTS[part][1]
        ids = ids_ref[part]
        dest = routing_ids(block[tokens : tokens + 8, 0:384])
        hit = ids == dest[0:1, :]
        for j in range(1, 8):
            hit = jnp.logical_or(hit, ids == dest[j : j + 1, :])
        onehot = jnp.where(hit, 1.0, 0.0).astype(jnp.bfloat16)
        rows = jnp.dot(onehot, block[0:tokens, :], preferred_element_type=jnp.float32).astype(jnp.bfloat16)
        chosen[n][part][:, off2, off1] = rows.reshape(8, SLOTS, width)

    def select_group(n, part, off2):
        start, width, _ = PARTS[part]
        plane = planes[n][part]
        if off2 == 0:
            meta_refs[n][part, 0] = own_refs[n][tokens : tokens + 8, start : start + 384]
            for off1 in range(1, RING):
                meta_refs[n][part, off1] = plane[off1, tokens : tokens + 8, 0:384]
            select(n, part, 0, 0, own_refs[n].at[:, start : start + width])
            first = 1
        else:
            for off1 in range(RING):
                drain(plane.at[off2 * RING + off1], plane_recv.at[n, part, off2 * RING + off1])
            first = 0

        def body(off1, carry):
            select(n, part, off2, off1, plane.at[off2 * RING + off1])
            return carry

        lax.fori_loop(first, RING, body, 0)

    def send_group(n, part, off2):
        s3 = PARTS[part][2][2]
        for i in (2, 3, 6, 7, 4, 5, 1):
            off3, flip = PAIRS[i]
            send(chosen[n][part].at[i, off2], group_view(out_refs[n], part, off3, flip, off2), row_send.at[n, part], row_recv.at[n], peer(s3, off3, flip)).start()
        pltpu.make_async_copy(chosen[n][part].at[0, off2], group_view(out_refs[n], part, 0, 0, off2), local_sem.at[n, part]).start()

    forward(0)
    for n in range(batches):
        late = None
        for off2 in (0, 1, 3, 2):
            for part in range(3):
                select_group(n, part, off2)
                if late is not None:
                    send_group(*late)
                late = (n, part, off2)
            if n == 0 and off2 == 0:
                forward(1)
        send_group(*late)

    for n in range(batches):
        drain(out_refs[n].at[1:8], row_recv.at[n])
        for part in range(3):
            plane = planes[n][part]
            drain(plane.at[1:16], plane_send.at[n, part])
            drain(chosen[n][part].at[1:8], row_send.at[n, part])
            drain(chosen[n][part].at[0], local_sem.at[n, part])


def dispatch(own_a, own_b, ids):
    rows, model = own_a.shape
    out = jax.ShapeDtypeStruct((CORES * RING, RING, RING, SLOTS, model), jnp.bfloat16)
    meta = jax.ShapeDtypeStruct((3, RING, 8, 384), jnp.bfloat16)
    any_spec, vmem_spec = pl.BlockSpec(memory_space=pl.ANY), pl.BlockSpec(memory_space=pltpu.VMEM)
    plane = [pltpu.VMEM((RING * RING, rows, width), jnp.bfloat16) for _, width, _ in PARTS]
    chosen = [pltpu.VMEM((8, RING, RING, SLOTS, width), jnp.bfloat16) for _, width, _ in PARTS]
    dma = pltpu.SemaphoreType.DMA
    return pl.pallas_call(
        dispatch_kernel,
        out_shape=(out, out, meta, meta),
        in_specs=[vmem_spec] * 3,
        out_specs=(any_spec, any_spec, vmem_spec, vmem_spec),
        scratch_shapes=plane * 2 + chosen * 2 + [dma((2, 3, 16)), dma((2, 3)), dma((2,)), dma((2, 3)), dma((2, 3))],
        compiler_params=pltpu.CompilerParams(collective_id=0, has_side_effects=True, vmem_limit_bytes=56 * 1024 * 1024),
        name="dispatch_rows",
    )(ids, own_a, own_b)


def return_kernel(ids_ref, *refs):
    batches = 2
    out_refs, meta_refs, res_refs, y_refs = refs[0:2], refs[2:4], refs[4:6], refs[6:8]
    scratch = refs[8:]
    back = [scratch[0 + 3 * n : 3 + 3 * n] for n in range(batches)]
    rows = [scratch[6 + 3 * n : 9 + 3 * n] for n in range(batches)]
    sums = [scratch[12 + 3 * n : 15 + 3 * n] for n in range(batches)]
    got = [scratch[18 + 3 * n : 21 + 3 * n] for n in range(batches)]
    back_recv, back_send, own_sem, rows_recv, rows_send, sums_recv, sums_send = scratch[24:]
    tokens = y_refs[0].shape[0]
    enter()

    for n in range(batches):
        for part in range(3):
            for off2 in range(RING):
                pltpu.make_async_copy(group_view(out_refs[n], part, 0, 0, off2), back[n][part].at[0, off2], own_sem.at[n, part]).start()
        for off2 in (2, 1, 3, 0):
            for i in (2, 3, 6, 7, 4, 5, 1):
                off3, flip = PAIRS[i]
                for part in range(3):
                    s3 = PARTS[part][2][2]
                    send(group_view(out_refs[n], part, off3, flip, off2), back[n][part].at[i, off2], back_send.at[n, part], back_recv.at[n, part, off2], peer(s3, -off3, flip)).start()

    def turn(n, off2):
        for part in range(3):
            s2 = PARTS[part][2][1]
            drain(back[n][part].at[1:8, off2], back_recv.at[n, part, off2])
            if off2:
                send(back[n][part].at[:, off2], rows[n][part].at[off2 - 1], rows_send.at[n, part], rows_recv.at[n, part, off2 - 1], peer(s2, -off2)).start()

    def weighted(n, part, off1):
        width = PARTS[part][1]
        meta = meta_refs[n][part, off1]
        dest = routing_ids(meta)
        gates = meta[:, 256:384].astype(jnp.float32)
        total = None
        for off2 in range(RING):
            ids = ids_ref[part, off2 * 128 : (off2 + 1) * 128, :]
            weight = jnp.zeros((128, tokens), jnp.float32)
            for j in range(8):
                weight = jnp.where(ids == dest[j : j + 1, :], gates[j : j + 1, :], weight)
            block = back[n][part][:, 0, off1] if off2 == 0 else rows[n][part][off2 - 1, :, off1]
            term = lax.dot_general(weight.astype(jnp.bfloat16), block.reshape(128, width), (((0,), (0,)), ((), ())), preferred_element_type=jnp.float32)
            total = term if total is None else total + term
        return total

    def own_ready(n):
        for part in range(3):
            drain(back[n][part].at[0], own_sem.at[n, part])

    def combine(n):
        for part in range(3):
            start, width, (s1, _, _) = PARTS[part]
            for off2 in (1, 3, 2):
                drain(rows[n][part].at[off2 - 1], rows_recv.at[n, part, off2 - 1])
            for off1 in (2, 1, 3):
                sums[n][part][off1 - 1] = weighted(n, part, off1)
            y_refs[n][:, start : start + width] = res_refs[n][:, start : start + width].astype(jnp.float32) + weighted(n, part, 0)
            for off1 in (2, 1, 3):
                send(sums[n][part].at[off1 - 1], got[n][part].at[off1 - 1], sums_send.at[n, part], sums_recv.at[n, part, off1 - 1], peer(s1, -off1)).start()

    def finish(n):
        for part in range(3):
            start, width, _ = PARTS[part]
            total = y_refs[n][:, start : start + width]
            for off1 in range(1, RING):
                drain(got[n][part].at[off1 - 1], sums_recv.at[n, part, off1 - 1])
                total = total + got[n][part][off1 - 1]
            y_refs[n][:, start : start + width] = total

    own_ready(0)
    for off2 in (2, 1, 3, 0):
        turn(0, off2)
    own_ready(1)
    turn(1, 2)
    combine(0)
    for off2 in (1, 3, 0):
        turn(1, off2)
    finish(0)
    combine(1)
    finish(1)
    for n in range(batches):
        for part in range(3):
            drain(back[n][part].at[1:8], back_send.at[n, part])
            drain(rows[n][part], rows_send.at[n, part])
            drain(sums[n][part], sums_send.at[n, part])


def bring_back(ids, outs, metas, residuals):
    tokens, model = residuals[0].shape
    y = jax.ShapeDtypeStruct((tokens, model), jnp.float32)
    any_spec, vmem_spec = pl.BlockSpec(memory_space=pl.ANY), pl.BlockSpec(memory_space=pltpu.VMEM)
    widths = [width for _, width, _ in PARTS]
    back = [pltpu.VMEM((8, RING, RING, SLOTS, width), jnp.bfloat16) for width in widths]
    rows = [pltpu.VMEM((RING - 1, 8, RING, SLOTS, width), jnp.bfloat16) for width in widths]
    sums = [pltpu.VMEM((RING - 1, tokens, width), jnp.float32) for width in widths]
    dma = pltpu.SemaphoreType.DMA
    return pl.pallas_call(
        return_kernel,
        out_shape=(y, y),
        in_specs=[vmem_spec] + [any_spec] * 2 + [vmem_spec] * 4,
        out_specs=(vmem_spec, vmem_spec),
        scratch_shapes=back * 2 + rows * 2 + sums * 2 + sums * 2
        + [dma((2, 3, RING)), dma((2, 3)), dma((2, 3)), dma((2, 3, 3)), dma((2, 3)), dma((2, 3, 3)), dma((2, 3))],
        compiler_params=pltpu.CompilerParams(collective_id=1, has_side_effects=True, vmem_limit_bytes=60 * 1024 * 1024),
        name="return_rows",
    )(ids, *outs, *metas, *residuals)


def ffn_kernel(x_ref, wg_ref, wu_ref, wd_ref, o_ref):
    x = x_ref[...].reshape(-1, wg_ref.shape[0])
    gate_act = jnp.dot(x, wg_ref[...], preferred_element_type=jnp.float32)
    up_act = jnp.dot(x, wu_ref[...], preferred_element_type=jnp.float32)
    hidden = (jax.nn.silu(gate_act) * up_act).astype(jnp.bfloat16)
    o_ref[...] = jnp.dot(hidden, wd_ref[...], preferred_element_type=jnp.float32).astype(jnp.bfloat16).reshape(o_ref.shape)


def expert_ffn(x, w_gate, w_up, w_down):
    model, ffn = w_gate.shape
    block = pl.BlockSpec((1,) + x.shape[1:], lambda i: (i, 0, 0, 0, 0))
    return pl.pallas_call(
        ffn_kernel,
        grid=(RING * CORES,),
        out_shape=jax.ShapeDtypeStruct(x.shape, x.dtype),
        in_specs=[block, pl.BlockSpec((model, ffn), lambda i: (0, 0)), pl.BlockSpec((model, ffn), lambda i: (0, 0)), pl.BlockSpec((ffn, model), lambda i: (0, 0))],
        out_specs=block,
        compiler_params=pltpu.CompilerParams(vmem_limit_bytes=40 * 1024 * 1024),
        cost_estimate=pl.CostEstimate(flops=6 * 2048 * model * ffn, bytes_accessed=26 * 1024 * 1024, transcendentals=2048 * ffn),
        name="expert_ffn",
    )(x, w_gate, w_up, w_down)


def token_rows(normed, experts, slots, gates):
    routing = jnp.concatenate([experts.T.astype(jnp.bfloat16), slots.T.astype(jnp.bfloat16), gates.T], axis=1)
    below = jnp.concatenate([jnp.pad(routing, ((0, 0), (0, width - routing.shape[1]))) for _, width, _ in PARTS], axis=1)
    return jnp.concatenate([normed, below], axis=0)


def solution(mesh):
    row_spec = P(("dp", "ep"), None)
    full_spec = P(None, None, None)
    gain_spec = P(None)
    expert_spec = P("ep", None, None)
    in_specs = (row_spec,) * 8 + (gain_spec,) + (full_spec,) * 4 + (gain_spec,) + (expert_spec,) * 3

    def device_fn(tokens_a, experts_a, slots_a, gates_a, tokens_b, experts_b, slots_b, gates_b, attn_gain, w_query, w_key, w_value, w_out, moe_gain, w_gate, w_up, w_down):
        w_gate, w_up, w_down = w_gate[0], w_up[0], w_down[0]
        ids = jnp.stack([row_ids(order) for _, _, order in PARTS])

        def front(tokens, experts, slots, gates):
            residual = attention_block(tokens, attn_gain, w_query, w_key, w_value, w_out)
            return residual, token_rows(rms_norm(residual, moe_gain), experts, slots, gates)

        res_a, own_a = front(tokens_a, experts_a, slots_a, gates_a)
        res_b, own_b = front(tokens_b, experts_b, slots_b, gates_b)
        x_a, x_b, meta_a, meta_b = dispatch(own_a, own_b, ids[:, :128])
        o_a = expert_ffn(x_a, w_gate, w_up, w_down)
        o_b = expert_ffn(x_b, w_gate, w_up, w_down)
        y_a, y_b = bring_back(ids, (o_a, o_b), (meta_a, meta_b), (res_a, res_b))
        return y_a.astype(jnp.bfloat16), y_b.astype(jnp.bfloat16)

    return jax.shard_map(device_fn, mesh=mesh, in_specs=in_specs, out_specs=(row_spec, row_spec), check_vma=False)
```

```python
import jax
import jax.numpy as jnp
from jax import lax
from jax.experimental import pallas as pl
from jax.experimental.pallas import tpu as pltpu
from jax.sharding import PartitionSpec as P

NORM_EPS = 1e-6
MASK_VALUE = -1e30
RING = 4
CORES = 2
SLOTS = 16
HEAD_DIM = 64
PARTS = (
    (0, 640, ("z", "y", "x")),
    (640, 640, ("x", "z", "y")),
    (1280, 768, ("y", "x", "z")),
)
STRIDE = {"z": 32, "y": 8, "x": 2}

def coords(index):
    return {"z": index // 32, "y": (index // 8) % RING, "x": (index // 2) % RING}, index % CORES


def attention_kernel(xa_ref, xb_ref, ea_ref, sa_ref, ga_ref, eb_ref, sb_ref, gb_ref, attn_gain_ref, moe_gain_ref, wq_ref, wk_ref, wv_ref, wo_ref, res_a_ref, res_b_ref, own_a_ref, own_b_ref, normed_t, total):
    step = pl.program_id(0)
    tokens = xa_ref.shape[0]
    xs = (xa_ref, xb_ref)

    def norm(rows_f, gain_ref):
        inv_rms = lax.rsqrt(jnp.mean(rows_f * rows_f, axis=-1, keepdims=True) + NORM_EPS)
        return rows_f * inv_rms * gain_ref[...].astype(jnp.float32)

    @pl.when(step == 0)
    def _():
        for n, x_ref in enumerate(xs):
            normed_t[:, n * tokens : (n + 1) * tokens] = norm(x_ref[...].astype(jnp.float32), attn_gain_ref).T.astype(jnp.bfloat16)
        total[...] = jnp.zeros_like(total)

    query, keys, values = (jnp.dot(w_ref[...], normed_t[...], preferred_element_type=jnp.float32).astype(jnp.bfloat16) for w_ref in (wq_ref, wk_ref, wv_ref))
    seen = lax.broadcasted_iota(jnp.int32, (tokens, tokens), 0) <= lax.broadcasted_iota(jnp.int32, (tokens, tokens), 1)
    contexts = []
    for n in range(2):
        parts = []
        for start in range(0, query.shape[0], HEAD_DIM):
            rows, cols = slice(start, start + HEAD_DIM), slice(n * tokens, (n + 1) * tokens)
            scores = lax.dot_general(keys[rows, cols], query[rows, cols], (((0,), (0,)), ((), ())), preferred_element_type=jnp.float32) * (HEAD_DIM**-0.5)
            scores = jnp.where(seen, scores, MASK_VALUE)
            weight = jnp.exp(scores - jnp.max(scores, axis=0, keepdims=True))
            prob = (weight / jnp.sum(weight, axis=0, keepdims=True)).astype(jnp.bfloat16)
            parts.append(jnp.dot(values[rows, cols], prob, preferred_element_type=jnp.float32).astype(jnp.bfloat16))
        contexts.append(jnp.concatenate(parts, axis=0))
    context = jnp.concatenate(contexts, axis=1)
    total[...] += lax.dot_general(context, wo_ref[...], (((0,), (0,)), ((), ())), preferred_element_type=jnp.float32)

    @pl.when(step == pl.num_programs(0) - 1)
    def _():
        routing = ((ea_ref, sa_ref, ga_ref), (eb_ref, sb_ref, gb_ref))
        for n, (x_ref, res_ref, own_ref) in enumerate(zip(xs, (res_a_ref, res_b_ref), (own_a_ref, own_b_ref))):
            residual = (x_ref[...].astype(jnp.float32) + total[n * tokens : (n + 1) * tokens, :]).astype(jnp.bfloat16)
            res_ref[...] = residual
            own_ref[0:tokens, :] = norm(residual.astype(jnp.float32), moe_gain_ref).astype(jnp.bfloat16)
            own_ref[tokens : tokens + 8, :] = jnp.zeros((8, own_ref.shape[1]), jnp.bfloat16)
            for start, _, _ in PARTS:
                for i, ref in enumerate(routing[n]):
                    own_ref[tokens : tokens + 8, start + i * 128 : start + (i + 1) * 128] = ref[...].astype(jnp.float32).astype(jnp.bfloat16)


def attention(tokens_a, routing_a, tokens_b, routing_b, attn_gain, moe_gain, w_query, w_key, w_value, w_out):
    tokens, model = tokens_a.shape
    steps = 8
    width = model // steps
    whole = lambda shape: pl.BlockSpec(shape, lambda i: (0,) * len(shape))
    weight = pl.BlockSpec((width, model), lambda i: (i, 0))
    flip = lambda w: jnp.transpose(w, (1, 2, 0)).reshape(model, model)
    rows, choices, gain = (tokens, model), (8, tokens), (1, model)
    own = (tokens + 8, model)
    return pl.pallas_call(
        attention_kernel,
        grid=(steps,),
        out_shape=tuple(jax.ShapeDtypeStruct(shape, jnp.bfloat16) for shape in (rows, rows, own, own)),
        in_specs=[whole(rows)] * 2 + [whole(choices)] * 6 + [whole(gain)] * 2 + [weight] * 4,
        out_specs=(whole(rows), whole(rows), whole(own), whole(own)),
        scratch_shapes=[pltpu.VMEM((model, 2 * tokens), jnp.bfloat16), pltpu.VMEM((2 * tokens, model), jnp.float32)],
        compiler_params=pltpu.CompilerParams(vmem_limit_bytes=40 * 1024 * 1024),
        name="attention",
    )(
        tokens_a, tokens_b, *(r.T for r in routing_a), *(r.T for r in routing_b),
        attn_gain.reshape(gain), moe_gain.reshape(gain), flip(w_query), flip(w_key), flip(w_value), w_out.reshape(model, model),
    )


def row_ids(order):
    s1, s2, s3 = order
    pos, core = coords(lax.axis_index("ep"))
    row = jnp.arange(RING * RING * CORES * SLOTS, dtype=jnp.int32)
    slot = row % SLOTS
    flip = (row // SLOTS) % CORES
    off3 = (row // (SLOTS * CORES)) % RING
    off2 = row // (SLOTS * CORES * RING)
    line = {s1: pos[s1], s2: (pos[s2] + off2) % RING, s3: (pos[s3] + off3) % RING}
    expert = line["z"] * 32 + line["y"] * 8 + line["x"] * 2 + jnp.where(flip == 1, 1 - core, core)
    ids = (expert * SLOTS + slot).astype(jnp.float32)
    return jnp.broadcast_to(ids[:, None], (ids.shape[0], 128))


def peer(dim, delta, flip=0):
    me = lax.axis_index("ep")
    stride = STRIDE[dim]
    place = lax.rem(me // stride, RING)
    other = me + (lax.rem(place + delta % RING, RING) - place) * stride
    if flip:
        other = other + 1 - 2 * lax.rem(me, CORES)
    return {"ep": other}


def send(src, dst, send_sem, recv_sem, where):
    return pltpu.make_async_remote_copy(src_ref=src, dst_ref=dst, send_sem=send_sem, recv_sem=recv_sem, device_id=where, device_id_type=pl.DeviceIdType.MESH)


def drain(ref, sem):
    pltpu.make_async_copy(ref, ref, sem).wait()


def enter():
    barrier = pltpu.get_barrier_semaphore()
    count = 0
    for dim in ("x", "y", "z"):
        for delta in range(1, RING):
            for flip in range(CORES):
                pl.semaphore_signal(barrier, inc=1, device_id=peer(dim, delta, flip), device_id_type=pl.DeviceIdType.MESH)
                count += 1
    pl.semaphore_signal(barrier, inc=1, device_id=peer("x", 0, 1), device_id_type=pl.DeviceIdType.MESH)
    pl.semaphore_wait(barrier, count + 1)


def group_view(rows, part, off3, flip, off2):
    start, width, (_, s2, s3) = PARTS[part]
    place = {s3: off3, s2: off2}
    index = tuple(place.get(dim, slice(None)) for dim in ("y", "z"))
    line = flip * RING + place["x"] if "x" in place else slice(flip * RING, (flip + 1) * RING)
    return rows.at[line, index[0], index[1], :, start : start + width]


PAIRS = tuple((off, flip) for off in range(RING) for flip in range(CORES))


def routing_ids(meta):
    expert = meta[:, 0:128].astype(jnp.float32)
    slot = meta[:, 128:256].astype(jnp.float32)
    return jnp.where(slot >= 0, expert * SLOTS + slot, -1.0)


def dispatch_kernel(ids_ref, *refs):
    batches = 2
    own_refs, out_refs, meta_refs = refs[0:2], refs[2:4], refs[4:6]
    planes = [refs[6 + 3 * n : 9 + 3 * n] for n in range(batches)]
    chosen = [refs[12 + 3 * n : 15 + 3 * n] for n in range(batches)]
    plane_recv, plane_send, row_recv, row_send, local_sem = refs[18:]
    tokens = own_refs[0].shape[0] - 8
    enter()

    def own_part(n, part):
        start, width, _ = PARTS[part]
        return own_refs[n].at[:, start : start + width]

    for n in range(batches):
        for part, (_, _, (s1, s2, _)) in enumerate(PARTS):
            plane = planes[n][part]
            for off in (1, 3, 2):
                send(own_part(n, part), plane.at[off], plane_send.at[n, part], plane_recv.at[n, part, off], peer(s1, off)).start()
                send(own_part(n, part), plane.at[off * RING], plane_send.at[n, part], plane_recv.at[n, part, off * RING], peer(s2, off)).start()

    def forward(n):
        for part, (_, _, (s1, s2, _)) in enumerate(PARTS):
            plane = planes[n][part]
            for off1 in (1, 3, 2):
                drain(plane.at[off1], plane_recv.at[n, part, off1])
                for off2 in (1, 3, 2):
                    send(plane.at[off1], plane.at[off2 * RING + off1], plane_send.at[n, part], plane_recv.at[n, part, off2 * RING + off1], peer(s2, off2)).start()

    def select(n, part, off2, off1, block):
        width = PARTS[part][1]
        ids = ids_ref[part]
        dest = routing_ids(block[tokens : tokens + 8, 0:384])
        hit = ids == dest[0:1, :]
        for j in range(1, 8):
            hit = jnp.logical_or(hit, ids == dest[j : j + 1, :])
        onehot = jnp.where(hit, 1.0, 0.0).astype(jnp.bfloat16)
        rows = jnp.dot(onehot, block[0:tokens, :], preferred_element_type=jnp.float32).astype(jnp.bfloat16)
        chosen[n][part][:, off2, off1] = rows.reshape(8, SLOTS, width)

    def select_group(n, part, off2):
        start, width, _ = PARTS[part]
        plane = planes[n][part]
        if off2 == 0:
            meta_refs[n][part, 0] = own_refs[n][tokens : tokens + 8, start : start + 384]
            for off1 in range(1, RING):
                meta_refs[n][part, off1] = plane[off1, tokens : tokens + 8, 0:384]
            select(n, part, 0, 0, own_refs[n].at[:, start : start + width])
            first = 1
        else:
            for off1 in range(RING):
                drain(plane.at[off2 * RING + off1], plane_recv.at[n, part, off2 * RING + off1])
            first = 0

        def body(off1, carry):
            select(n, part, off2, off1, plane.at[off2 * RING + off1])
            return carry

        lax.fori_loop(first, RING, body, 0)

    def send_group(n, part, off2):
        s3 = PARTS[part][2][2]
        for i in (2, 3, 6, 7, 4, 5, 1):
            off3, flip = PAIRS[i]
            send(chosen[n][part].at[i, off2], group_view(out_refs[n], part, off3, flip, off2), row_send.at[n, part], row_recv.at[n], peer(s3, off3, flip)).start()
        pltpu.make_async_copy(chosen[n][part].at[0, off2], group_view(out_refs[n], part, 0, 0, off2), local_sem.at[n, part]).start()

    forward(0)
    for n in range(batches):
        late = None
        for off2 in (0, 1, 3, 2):
            for part in range(3):
                select_group(n, part, off2)
                if late is not None:
                    send_group(*late)
                late = (n, part, off2)
            if n == 0 and off2 == 0:
                forward(1)
        send_group(*late)

    for n in range(batches):
        drain(out_refs[n].at[1:8], row_recv.at[n])
        for part in range(3):
            plane = planes[n][part]
            drain(plane.at[1:16], plane_send.at[n, part])
            drain(chosen[n][part].at[1:8], row_send.at[n, part])
            drain(chosen[n][part].at[0], local_sem.at[n, part])


def dispatch(own_a, own_b, ids):
    rows, model = own_a.shape
    out = jax.ShapeDtypeStruct((CORES * RING, RING, RING, SLOTS, model), jnp.bfloat16)
    meta = jax.ShapeDtypeStruct((3, RING, 8, 384), jnp.bfloat16)
    any_spec, vmem_spec = pl.BlockSpec(memory_space=pl.ANY), pl.BlockSpec(memory_space=pltpu.VMEM)
    plane = [pltpu.VMEM((RING * RING, rows, width), jnp.bfloat16) for _, width, _ in PARTS]
    chosen = [pltpu.VMEM((8, RING, RING, SLOTS, width), jnp.bfloat16) for _, width, _ in PARTS]
    dma = pltpu.SemaphoreType.DMA
    return pl.pallas_call(
        dispatch_kernel,
        out_shape=(out, out, meta, meta),
        in_specs=[vmem_spec] * 3,
        out_specs=(any_spec, any_spec, vmem_spec, vmem_spec),
        scratch_shapes=plane * 2 + chosen * 2 + [dma((2, 3, 16)), dma((2, 3)), dma((2,)), dma((2, 3)), dma((2, 3))],
        compiler_params=pltpu.CompilerParams(collective_id=0, has_side_effects=True, vmem_limit_bytes=56 * 1024 * 1024),
        name="dispatch_rows",
    )(ids, own_a, own_b)


def return_kernel(ids_ref, *refs):
    batches = 2
    out_refs, meta_refs, res_refs, y_refs = refs[0:2], refs[2:4], refs[4:6], refs[6:8]
    scratch = refs[8:]
    back = [scratch[0 + 3 * n : 3 + 3 * n] for n in range(batches)]
    rows = [scratch[6 + 3 * n : 9 + 3 * n] for n in range(batches)]
    sums = [scratch[12 + 3 * n : 15 + 3 * n] for n in range(batches)]
    got = [scratch[18 + 3 * n : 21 + 3 * n] for n in range(batches)]
    back_recv, back_send, own_sem, rows_recv, rows_send, sums_recv, sums_send = scratch[24:]
    tokens = y_refs[0].shape[0]
    enter()

    for n in range(batches):
        for part in range(3):
            for off2 in range(RING):
                pltpu.make_async_copy(group_view(out_refs[n], part, 0, 0, off2), back[n][part].at[0, off2], own_sem.at[n, part]).start()
        for off2 in (2, 1, 3, 0):
            for i in (2, 3, 6, 7, 4, 5, 1):
                off3, flip = PAIRS[i]
                for part in range(3):
                    s3 = PARTS[part][2][2]
                    send(group_view(out_refs[n], part, off3, flip, off2), back[n][part].at[i, off2], back_send.at[n, part], back_recv.at[n, part, off2], peer(s3, -off3, flip)).start()

    def turn(n, off2):
        for part in range(3):
            s2 = PARTS[part][2][1]
            drain(back[n][part].at[1:8, off2], back_recv.at[n, part, off2])
            if off2:
                send(back[n][part].at[:, off2], rows[n][part].at[off2 - 1], rows_send.at[n, part], rows_recv.at[n, part, off2 - 1], peer(s2, -off2)).start()

    def weighted(n, part, off1):
        width = PARTS[part][1]
        meta = meta_refs[n][part, off1]
        dest = routing_ids(meta)
        gates = meta[:, 256:384].astype(jnp.float32)
        total = None
        for off2 in range(RING):
            ids = ids_ref[part, off2 * 128 : (off2 + 1) * 128, :]
            weight = jnp.zeros((128, tokens), jnp.float32)
            for j in range(8):
                weight = jnp.where(ids == dest[j : j + 1, :], gates[j : j + 1, :], weight)
            block = back[n][part][:, 0, off1] if off2 == 0 else rows[n][part][off2 - 1, :, off1]
            term = lax.dot_general(weight.astype(jnp.bfloat16), block.reshape(128, width), (((0,), (0,)), ((), ())), preferred_element_type=jnp.float32)
            total = term if total is None else total + term
        return total

    def own_ready(n):
        for part in range(3):
            drain(back[n][part].at[0], own_sem.at[n, part])

    def combine(n):
        for part in range(3):
            start, width, (s1, _, _) = PARTS[part]
            for off2 in (1, 3, 2):
                drain(rows[n][part].at[off2 - 1], rows_recv.at[n, part, off2 - 1])
            for off1 in (2, 1, 3):
                sums[n][part][off1 - 1] = weighted(n, part, off1)
            y_refs[n][:, start : start + width] = res_refs[n][:, start : start + width].astype(jnp.float32) + weighted(n, part, 0)
            for off1 in (2, 1, 3):
                send(sums[n][part].at[off1 - 1], got[n][part].at[off1 - 1], sums_send.at[n, part], sums_recv.at[n, part, off1 - 1], peer(s1, -off1)).start()

    def finish(n):
        for part in range(3):
            start, width, _ = PARTS[part]
            total = y_refs[n][:, start : start + width]
            for off1 in range(1, RING):
                drain(got[n][part].at[off1 - 1], sums_recv.at[n, part, off1 - 1])
                total = total + got[n][part][off1 - 1]
            y_refs[n][:, start : start + width] = total

    own_ready(0)
    for off2 in (2, 1, 3, 0):
        turn(0, off2)
    own_ready(1)
    turn(1, 2)
    combine(0)
    for off2 in (1, 3, 0):
        turn(1, off2)
    finish(0)
    combine(1)
    finish(1)
    for n in range(batches):
        for part in range(3):
            drain(back[n][part].at[1:8], back_send.at[n, part])
            drain(rows[n][part], rows_send.at[n, part])
            drain(sums[n][part], sums_send.at[n, part])


def bring_back(ids, outs, metas, residuals):
    tokens, model = residuals[0].shape
    y = jax.ShapeDtypeStruct((tokens, model), jnp.float32)
    any_spec, vmem_spec = pl.BlockSpec(memory_space=pl.ANY), pl.BlockSpec(memory_space=pltpu.VMEM)
    widths = [width for _, width, _ in PARTS]
    back = [pltpu.VMEM((8, RING, RING, SLOTS, width), jnp.bfloat16) for width in widths]
    rows = [pltpu.VMEM((RING - 1, 8, RING, SLOTS, width), jnp.bfloat16) for width in widths]
    sums = [pltpu.VMEM((RING - 1, tokens, width), jnp.float32) for width in widths]
    dma = pltpu.SemaphoreType.DMA
    return pl.pallas_call(
        return_kernel,
        out_shape=(y, y),
        in_specs=[vmem_spec] + [any_spec] * 2 + [vmem_spec] * 4,
        out_specs=(vmem_spec, vmem_spec),
        scratch_shapes=back * 2 + rows * 2 + sums * 2 + sums * 2
        + [dma((2, 3, RING)), dma((2, 3)), dma((2, 3)), dma((2, 3, 3)), dma((2, 3)), dma((2, 3, 3)), dma((2, 3))],
        compiler_params=pltpu.CompilerParams(collective_id=1, has_side_effects=True, vmem_limit_bytes=60 * 1024 * 1024),
        name="return_rows",
    )(ids, *outs, *metas, *residuals)


def ffn_kernel(x_ref, wg_ref, wu_ref, wd_ref, o_ref):
    x = x_ref[...].reshape(-1, wg_ref.shape[0])
    gate_act = jnp.dot(x, wg_ref[...], preferred_element_type=jnp.float32)
    up_act = jnp.dot(x, wu_ref[...], preferred_element_type=jnp.float32)
    hidden = (jax.nn.silu(gate_act) * up_act).astype(jnp.bfloat16)
    o_ref[...] = jnp.dot(hidden, wd_ref[...], preferred_element_type=jnp.float32).astype(jnp.bfloat16).reshape(o_ref.shape)


def expert_ffn(x, w_gate, w_up, w_down):
    model, ffn = w_gate.shape
    block = pl.BlockSpec((1,) + x.shape[1:], lambda i: (i, 0, 0, 0, 0))
    return pl.pallas_call(
        ffn_kernel,
        grid=(RING * CORES,),
        out_shape=jax.ShapeDtypeStruct(x.shape, x.dtype),
        in_specs=[block, pl.BlockSpec((model, ffn), lambda i: (0, 0)), pl.BlockSpec((model, ffn), lambda i: (0, 0)), pl.BlockSpec((ffn, model), lambda i: (0, 0))],
        out_specs=block,
        compiler_params=pltpu.CompilerParams(vmem_limit_bytes=40 * 1024 * 1024),
        cost_estimate=pl.CostEstimate(flops=6 * 2048 * model * ffn, bytes_accessed=26 * 1024 * 1024, transcendentals=2048 * ffn),
        name="expert_ffn",
    )(x, w_gate, w_up, w_down)


def solution(mesh):
    row_spec = P(("dp", "ep"), None)
    full_spec = P(None, None, None)
    gain_spec = P(None)
    expert_spec = P("ep", None, None)
    in_specs = (row_spec,) * 8 + (gain_spec,) + (full_spec,) * 4 + (gain_spec,) + (expert_spec,) * 3

    def device_fn(tokens_a, experts_a, slots_a, gates_a, tokens_b, experts_b, slots_b, gates_b, attn_gain, w_query, w_key, w_value, w_out, moe_gain, w_gate, w_up, w_down):
        w_gate, w_up, w_down = w_gate[0], w_up[0], w_down[0]
        ids = jnp.stack([row_ids(order) for _, _, order in PARTS])

        res_a, res_b, own_a, own_b = attention(
            tokens_a, (experts_a, slots_a, gates_a), tokens_b, (experts_b, slots_b, gates_b), attn_gain, moe_gain, w_query, w_key, w_value, w_out
        )
        x_a, x_b, meta_a, meta_b = dispatch(own_a, own_b, ids[:, :128])
        o_a = expert_ffn(x_a, w_gate, w_up, w_down)
        o_b = expert_ffn(x_b, w_gate, w_up, w_down)
        y_a, y_b = bring_back(ids, (o_a, o_b), (meta_a, meta_b), (res_a, res_b))
        return y_a.astype(jnp.bfloat16), y_b.astype(jnp.bfloat16)

    return jax.shard_map(device_fn, mesh=mesh, in_specs=in_specs, out_specs=(row_spec, row_spec), check_vma=False)
```

```python
import jax
import jax.numpy as jnp
from jax import lax
from jax.experimental import pallas as pl
from jax.experimental.pallas import tpu as pltpu
from jax.sharding import PartitionSpec as P

NORM_EPS = 1e-6
MASK_VALUE = -1e30
RING = 4
CORES = 2
SLOTS = 16
HEAD_DIM = 64
PARTS = (
    (0, 640, ("z", "y", "x")),
    (640, 640, ("x", "z", "y")),
    (1280, 768, ("y", "x", "z")),
)
STRIDE = {"z": 32, "y": 8, "x": 2}

def coords(index):
    return {"z": index // 32, "y": (index // 8) % RING, "x": (index // 2) % RING}, index % CORES


def attention_kernel(xa_ref, xb_ref, ea_ref, sa_ref, ga_ref, eb_ref, sb_ref, gb_ref, attn_gain_ref, moe_gain_ref, wq_ref, wk_ref, wv_ref, wo_ref, res_a_ref, res_b_ref, own_a_ref, own_b_ref, normed_t, total):
    step = pl.program_id(0)
    tokens = xa_ref.shape[0]
    xs = (xa_ref, xb_ref)

    def norm(rows_f, gain_ref):
        inv_rms = lax.rsqrt(jnp.mean(rows_f * rows_f, axis=-1, keepdims=True) + NORM_EPS)
        return rows_f * inv_rms * gain_ref[...].astype(jnp.float32).reshape(1, -1)

    @pl.when(step == 0)
    def _():
        for n, x_ref in enumerate(xs):
            normed_t[:, n * tokens : (n + 1) * tokens] = norm(x_ref[...].astype(jnp.float32), attn_gain_ref).T.astype(jnp.bfloat16)
        total[...] = jnp.zeros_like(total)

    query, keys, values = (jnp.dot(w_ref[...], normed_t[...], preferred_element_type=jnp.float32).astype(jnp.bfloat16) for w_ref in (wq_ref, wk_ref, wv_ref))
    seen = lax.broadcasted_iota(jnp.int32, (tokens, tokens), 0) <= lax.broadcasted_iota(jnp.int32, (tokens, tokens), 1)
    contexts = []
    for n in range(2):
        parts = []
        for start in range(0, query.shape[0], HEAD_DIM):
            rows, cols = slice(start, start + HEAD_DIM), slice(n * tokens, (n + 1) * tokens)
            scores = lax.dot_general(keys[rows, cols], query[rows, cols], (((0,), (0,)), ((), ())), preferred_element_type=jnp.float32) * (HEAD_DIM**-0.5)
            scores = jnp.where(seen, scores, MASK_VALUE)
            weight = jnp.exp(scores - jnp.max(scores, axis=0, keepdims=True))
            prob = (weight / jnp.sum(weight, axis=0, keepdims=True)).astype(jnp.bfloat16)
            parts.append(jnp.dot(values[rows, cols], prob, preferred_element_type=jnp.float32).astype(jnp.bfloat16))
        contexts.append(jnp.concatenate(parts, axis=0))
    context = jnp.concatenate(contexts, axis=1)
    total[...] += lax.dot_general(context, wo_ref[...], (((0,), (0,)), ((), ())), preferred_element_type=jnp.float32)

    @pl.when(step == pl.num_programs(0) - 1)
    def _():
        routing = ((ea_ref, sa_ref, ga_ref), (eb_ref, sb_ref, gb_ref))
        for n, (x_ref, res_ref, own_ref) in enumerate(zip(xs, (res_a_ref, res_b_ref), (own_a_ref, own_b_ref))):
            residual = (x_ref[...].astype(jnp.float32) + total[n * tokens : (n + 1) * tokens, :]).astype(jnp.bfloat16)
            res_ref[...] = residual
            own_ref[0:tokens, :] = norm(residual.astype(jnp.float32), moe_gain_ref).astype(jnp.bfloat16)
            own_ref[tokens : tokens + 8, :] = jnp.zeros((8, own_ref.shape[1]), jnp.bfloat16)
            for start, _, _ in PARTS:
                for i, ref in enumerate(routing[n]):
                    own_ref[tokens : tokens + 8, start + i * 128 : start + (i + 1) * 128] = ref[...].astype(jnp.float32).astype(jnp.bfloat16)


def attention(tokens_a, routing_a, tokens_b, routing_b, attn_gain, moe_gain, w_query, w_key, w_value, w_out):
    tokens, model = tokens_a.shape
    steps = 8
    width = model // steps
    whole = lambda shape: pl.BlockSpec(shape, lambda i: (0,) * len(shape))
    weight = pl.BlockSpec((width, model), lambda i: (i, 0))
    flip = lambda w: jnp.transpose(w, (1, 2, 0)).reshape(model, model)
    rows, choices, gain = (tokens, model), (8, tokens), (model,)
    own = (tokens + 8, model)
    return pl.pallas_call(
        attention_kernel,
        grid=(steps,),
        out_shape=tuple(jax.ShapeDtypeStruct(shape, jnp.bfloat16) for shape in (rows, rows, own, own)),
        in_specs=[whole(rows)] * 2 + [whole(choices)] * 6 + [whole(gain)] * 2 + [weight] * 4,
        out_specs=(whole(rows), whole(rows), whole(own), whole(own)),
        scratch_shapes=[pltpu.VMEM((model, 2 * tokens), jnp.bfloat16), pltpu.VMEM((2 * tokens, model), jnp.float32)],
        compiler_params=pltpu.CompilerParams(vmem_limit_bytes=62 * 1024 * 1024),
        name="attention",
    )(
        tokens_a, tokens_b, *(r.T for r in routing_a), *(r.T for r in routing_b),
        attn_gain, moe_gain, flip(w_query), flip(w_key), flip(w_value), w_out.reshape(model, model),
    )


def row_ids(order):
    s1, s2, s3 = order
    pos, core = coords(lax.axis_index("ep"))
    row = jnp.arange(RING * RING * CORES * SLOTS, dtype=jnp.int32)
    slot = row % SLOTS
    flip = (row // SLOTS) % CORES
    off3 = (row // (SLOTS * CORES)) % RING
    off2 = row // (SLOTS * CORES * RING)
    line = {s1: pos[s1], s2: (pos[s2] + off2) % RING, s3: (pos[s3] + off3) % RING}
    expert = line["z"] * 32 + line["y"] * 8 + line["x"] * 2 + jnp.where(flip == 1, 1 - core, core)
    ids = (expert * SLOTS + slot).astype(jnp.float32)
    return jnp.broadcast_to(ids[:, None], (ids.shape[0], 128))


def peer(dim, delta, flip=0):
    me = lax.axis_index("ep")
    stride = STRIDE[dim]
    place = lax.rem(me // stride, RING)
    other = me + (lax.rem(place + delta % RING, RING) - place) * stride
    if flip:
        other = other + 1 - 2 * lax.rem(me, CORES)
    return {"ep": other}


def send(src, dst, send_sem, recv_sem, where):
    return pltpu.make_async_remote_copy(src_ref=src, dst_ref=dst, send_sem=send_sem, recv_sem=recv_sem, device_id=where, device_id_type=pl.DeviceIdType.MESH)


def drain(ref, sem):
    pltpu.make_async_copy(ref, ref, sem).wait()


def enter():
    barrier = pltpu.get_barrier_semaphore()
    count = 0
    for dim in ("x", "y", "z"):
        for delta in range(1, RING):
            for flip in range(CORES):
                pl.semaphore_signal(barrier, inc=1, device_id=peer(dim, delta, flip), device_id_type=pl.DeviceIdType.MESH)
                count += 1
    pl.semaphore_signal(barrier, inc=1, device_id=peer("x", 0, 1), device_id_type=pl.DeviceIdType.MESH)
    pl.semaphore_wait(barrier, count + 1)


def group_view(rows, part, off3, flip, off2):
    start, width, (_, s2, s3) = PARTS[part]
    place = {s3: off3, s2: off2}
    index = tuple(place.get(dim, slice(None)) for dim in ("y", "z"))
    line = flip * RING + place["x"] if "x" in place else slice(flip * RING, (flip + 1) * RING)
    return rows.at[line, index[0], index[1], :, start : start + width]


PAIRS = tuple((off, flip) for off in range(RING) for flip in range(CORES))


def routing_ids(meta):
    expert = meta[:, 0:128].astype(jnp.float32)
    slot = meta[:, 128:256].astype(jnp.float32)
    return jnp.where(slot >= 0, expert * SLOTS + slot, -1.0)


def load_weights(w_refs, held, sem):
    copies = [pltpu.make_async_copy(src, dst, sem.at[i]) for i, (src, dst) in enumerate(zip(w_refs, held))]
    for copy in copies:
        copy.start()
    return copies


def run_experts(x_ref, o_ref, held, x_buf, o_buf, x_sem, o_sem, between):
    blocks = x_ref.shape[0]
    gate_w, up_w, down_w = held

    def load(b, slot):
        return pltpu.make_async_copy(x_ref.at[b], x_buf.at[slot], x_sem.at[slot])

    load(0, 0).start()

    def step(b, carry):
        slot = lax.rem(b, 2)

        @pl.when(b + 1 < blocks)
        def _():
            load(b + 1, 1 - slot).start()

        load(b, slot).wait()

        @pl.when(b >= 2)
        def _():
            drain(o_buf.at[slot], o_sem.at[slot])

        x = x_buf[slot].reshape(-1, gate_w.shape[0])
        gate_act = jnp.dot(x, gate_w[...], preferred_element_type=jnp.float32)
        up_act = jnp.dot(x, up_w[...], preferred_element_type=jnp.float32)
        hidden = (jax.nn.silu(gate_act) * up_act).astype(jnp.bfloat16)
        o_buf[slot] = jnp.dot(hidden, down_w[...], preferred_element_type=jnp.float32).astype(jnp.bfloat16).reshape(o_buf.shape[1:])
        pltpu.make_async_copy(o_buf.at[slot], o_ref.at[b], o_sem.at[slot]).start()
        between(b)
        return carry

    lax.fori_loop(0, blocks, step, 0)
    for slot in range(2):
        drain(o_buf.at[slot], o_sem.at[slot])


def expert_scratch(model, ffn):
    block = (2, RING, RING, SLOTS, model)
    dma = pltpu.SemaphoreType.DMA
    return [
        pltpu.VMEM((model, ffn), jnp.bfloat16),
        pltpu.VMEM((model, ffn), jnp.bfloat16),
        pltpu.VMEM((ffn, model), jnp.bfloat16),
        pltpu.VMEM(block, jnp.bfloat16),
        pltpu.VMEM(block, jnp.bfloat16),
        dma((3,)),
        dma((2,)),
        dma((2,)),
    ]


def dispatch_kernel(ids_ref, *refs):
    batches = 2
    own_refs, w_refs, out_refs, meta_refs, done_ref = refs[0:2], refs[2:5], refs[5:7], refs[7:9], refs[9]
    scratch = refs[10:]
    planes = [scratch[3 * n : 3 + 3 * n] for n in range(batches)]
    chosen = [scratch[6 + 3 * n : 9 + 3 * n] for n in range(batches)]
    plane_recv, plane_send, row_recv, row_send, local_sem = scratch[12:17]
    held, (x_buf, o_buf, w_sem, x_sem, o_sem) = scratch[17:20], scratch[20:]
    tokens = own_refs[0].shape[0] - 8
    half = tokens // 2
    enter()
    weight_copies = load_weights(w_refs, held, w_sem)

    def own_part(n, part):
        start, width, _ = PARTS[part]
        return own_refs[n].at[:, start : start + width]

    for n in range(batches):
        for part, (_, _, (s1, s2, _)) in enumerate(PARTS):
            plane = planes[n][part]
            for off in (1, 3, 2):
                send(own_part(n, part), plane.at[off], plane_send.at[n, part], plane_recv.at[n, part, off], peer(s1, off)).start()
            for off in (1, 3):
                send(own_part(n, part), plane.at[off * RING], plane_send.at[n, part], plane_recv.at[n, part, off * RING], peer(s2, off)).start()

    def forward(n):
        for part, (_, _, (s1, s2, _)) in enumerate(PARTS):
            plane = planes[n][part]
            for off1 in (1, 3, 2):
                drain(plane.at[off1], plane_recv.at[n, part, off1])
                for off2 in (1, 3):
                    send(plane.at[off1], plane.at[off2 * RING + off1], plane_send.at[n, part], plane_recv.at[n, part, off2 * RING + off1], peer(s2, off2)).start()

    def relay(n, off2):
        rows = slice(0, half) if off2 == 1 else slice(half, tokens + 8)
        for part, (_, _, (s1, s2, _)) in enumerate(PARTS):
            plane = planes[n][part]
            for off1 in range(RING):
                drain(plane.at[off2 * RING + off1], plane_recv.at[n, part, off2 * RING + off1])
                send(plane.at[off2 * RING + off1, rows], plane.at[2 * RING + off1, rows], plane_send.at[n, part], plane_recv.at[n, part, 2 * RING + off1], peer(s2, off2)).start()

    def select(n, part, off2, off1, block):
        width = PARTS[part][1]
        ids = ids_ref[part]
        dest = routing_ids(block[tokens : tokens + 8, 0:384])
        hit = ids == dest[0:1, :]
        for j in range(1, 8):
            hit = jnp.logical_or(hit, ids == dest[j : j + 1, :])
        onehot = jnp.where(hit, 1.0, 0.0).astype(jnp.bfloat16)
        rows = jnp.dot(onehot, block[0:tokens, :], preferred_element_type=jnp.float32).astype(jnp.bfloat16)
        chosen[n][part][:, off2, off1] = rows.reshape(8, SLOTS, width)

    def select_group(n, part, off2):
        start, width, _ = PARTS[part]
        plane = planes[n][part]
        if off2 == 0:
            meta_refs[n][part, 0] = own_refs[n][tokens : tokens + 8, start : start + 384]
            for off1 in range(1, RING):
                meta_refs[n][part, off1] = plane[off1, tokens : tokens + 8, 0:384]
            select(n, part, 0, 0, own_refs[n].at[:, start : start + width])
            first = 1
        else:
            for off1 in range(RING if off2 == 2 else 0):
                drain(plane.at[off2 * RING + off1], plane_recv.at[n, part, off2 * RING + off1])
            first = 0

        def body(off1, carry):
            select(n, part, off2, off1, plane.at[off2 * RING + off1])
            return carry

        lax.fori_loop(first, RING, body, 0)

    def send_group(n, part, off2):
        s3 = PARTS[part][2][2]
        for i in (2, 3, 6, 7, 4, 5, 1):
            off3, flip = PAIRS[i]
            send(chosen[n][part].at[i, off2], group_view(out_refs[n], part, off3, flip, off2), row_send.at[n, part], row_recv.at[n], peer(s3, off3, flip)).start()
        pltpu.make_async_copy(chosen[n][part].at[0, off2], group_view(out_refs[n], part, 0, 0, off2), local_sem.at[n, part]).start()

    late = []

    def groups(n, off2):
        for part in range(3):
            select_group(n, part, off2)
            if late:
                send_group(*late.pop())
            late.append((n, part, off2))

    forward(0)
    groups(0, 0)
    forward(1)
    relay(0, 1)
    relay(0, 3)
    groups(0, 1)
    groups(0, 3)
    relay(1, 1)
    relay(1, 3)
    groups(0, 2)
    for off2 in (0, 1, 3, 2):
        groups(1, off2)
    send_group(*late.pop())

    def rows_done(n):
        drain(out_refs[n].at[1:8], row_recv.at[n])
        for part in range(3):
            drain(chosen[n][part].at[0], local_sem.at[n, part])

    rows_done(0)
    for copy in weight_copies:
        copy.wait()
    run_experts(out_refs[0], done_ref, held, x_buf, o_buf, x_sem, o_sem, lambda b: None)
    rows_done(1)
    for n in range(batches):
        for part in range(3):
            drain(planes[n][part].at[1:16], plane_send.at[n, part])
            drain(chosen[n][part].at[1:8], row_send.at[n, part])


def dispatch(own_a, own_b, ids, weights):
    rows, model = own_a.shape
    ffn = weights[0].shape[1]
    out = jax.ShapeDtypeStruct((CORES * RING, RING, RING, SLOTS, model), jnp.bfloat16)
    meta = jax.ShapeDtypeStruct((3, RING, 8, 384), jnp.bfloat16)
    any_spec, vmem_spec = pl.BlockSpec(memory_space=pl.ANY), pl.BlockSpec(memory_space=pltpu.VMEM)
    plane = [pltpu.VMEM((RING * RING, rows, width), jnp.bfloat16) for _, width, _ in PARTS]
    chosen = [pltpu.VMEM((8, RING, RING, SLOTS, width), jnp.bfloat16) for _, width, _ in PARTS]
    dma = pltpu.SemaphoreType.DMA
    return pl.pallas_call(
        dispatch_kernel,
        out_shape=(out, out, meta, meta, out),
        in_specs=[vmem_spec] * 3 + [any_spec] * 3,
        out_specs=(any_spec, any_spec, vmem_spec, vmem_spec, any_spec),
        scratch_shapes=plane * 2 + chosen * 2 + [dma((2, 3, 16)), dma((2, 3)), dma((2,)), dma((2, 3)), dma((2, 3))] + expert_scratch(model, ffn),
        compiler_params=pltpu.CompilerParams(collective_id=0, has_side_effects=True, vmem_limit_bytes=62 * 1024 * 1024),
        name="dispatch_rows",
    )(ids, own_a, own_b, *weights)


def return_kernel(ids_ref, *refs):
    batches = 2
    done_a, x_b, meta_refs, res_refs, w_refs = refs[0], refs[1], refs[2:4], refs[4:6], refs[6:9]
    y_refs, done_b, scratch = refs[9:11], refs[11], refs[12:]
    out_refs = (done_a, done_b)
    back = [scratch[0 + 3 * n : 3 + 3 * n] for n in range(batches)]
    rows = [scratch[6 + 3 * n : 9 + 3 * n] for n in range(batches)]
    sums, got = scratch[12:15], [scratch[15 + 3 * n : 18 + 3 * n] for n in range(batches)]
    kept = scratch[21]
    back_recv, back_send, own_sem, rows_recv, rows_send, sums_recv, sums_send = scratch[22:29]
    held, (x_buf, o_buf, w_sem, x_sem, o_sem) = scratch[29:32], scratch[32:]
    tokens = y_refs[0].shape[0]
    enter()
    weight_copies = load_weights(w_refs, held, w_sem)

    def hand_out(n):
        for part in range(3):
            for off2 in range(RING):
                pltpu.make_async_copy(group_view(out_refs[n], part, 0, 0, off2), back[n][part].at[0, off2], own_sem.at[n, part]).start()
        for off2 in (2, 1, 3, 0):
            for i in (2, 3, 6, 7, 4, 5, 1):
                off3, flip = PAIRS[i]
                for part in range(3):
                    s3 = PARTS[part][2][2]
                    send(group_view(out_refs[n], part, off3, flip, off2), back[n][part].at[i, off2], back_send.at[n, part], back_recv.at[n, part, off2], peer(s3, -off3, flip)).start()

    def turn(n, off2):
        for part in range(3):
            s2 = PARTS[part][2][1]
            drain(back[n][part].at[1:8, off2], back_recv.at[n, part, off2])
            if off2:
                send(back[n][part].at[:, off2], rows[n][part].at[off2 - 1], rows_send.at[n, part], rows_recv.at[n, part, off2 - 1], peer(s2, -off2)).start()

    def weighted(n, part, off1):
        width = PARTS[part][1]
        meta = meta_refs[n][part, off1]
        dest = routing_ids(meta)
        gates = meta[:, 256:384].astype(jnp.float32)
        total = None
        for off2 in range(RING):
            ids = ids_ref[part, off2 * 128 : (off2 + 1) * 128, :]
            weight = jnp.zeros((128, tokens), jnp.float32)
            for j in range(8):
                weight = jnp.where(ids == dest[j : j + 1, :], gates[j : j + 1, :], weight)
            block = back[n][part][:, 0, off1] if off2 == 0 else rows[n][part][off2 - 1, :, off1]
            term = lax.dot_general(weight.astype(jnp.bfloat16), block.reshape(128, width), (((0,), (0,)), ((), ())), preferred_element_type=jnp.float32)
            total = term if total is None else total + term
        return total

    def own_ready(n):
        for part in range(3):
            drain(back[n][part].at[0], own_sem.at[n, part])

    def combine(n):
        for part in range(3):
            start, width, (s1, _, _) = PARTS[part]
            for off2 in (1, 3, 2):
                drain(rows[n][part].at[off2 - 1], rows_recv.at[n, part, off2 - 1])
            for off1 in (2, 1, 3):
                sums[part][off1 - 1] = weighted(n, part, off1)
            kept[:, start : start + width] = res_refs[n][:, start : start + width].astype(jnp.float32) + weighted(n, part, 0)
            for off1 in (2, 1, 3):
                send(sums[part].at[off1 - 1], got[n][part].at[off1 - 1], sums_send.at[part], sums_recv.at[n, part, off1 - 1], peer(s1, -off1)).start()

    def finish(n):
        for part in range(3):
            start, width, _ = PARTS[part]
            total = kept[:, start : start + width]
            for off1 in range(1, RING):
                drain(got[n][part].at[off1 - 1], sums_recv.at[n, part, off1 - 1])
                total = total + got[n][part][off1 - 1]
            y_refs[n][:, start : start + width] = total.astype(y_refs[n].dtype)
            drain(sums[part], sums_send.at[part])

    hand_out(0)
    for copy in weight_copies:
        copy.wait()

    def between(b):
        for when, off2 in ((1, 2), (3, 1), (5, 3), (7, 0)):

            @pl.when(b == when)
            def _():
                if off2 == 2:
                    own_ready(0)
                turn(0, off2)

    run_experts(x_b, done_b, held, x_buf, o_buf, x_sem, o_sem, between)
    hand_out(1)
    combine(0)
    own_ready(1)
    for off2 in (2, 1, 3, 0):
        turn(1, off2)
    finish(0)
    combine(1)
    finish(1)
    for n in range(batches):
        for part in range(3):
            drain(back[n][part].at[1:8], back_send.at[n, part])
            drain(rows[n][part], rows_send.at[n, part])


def bring_back(ids, done_a, x_b, metas, residuals, weights):
    tokens, model = residuals[0].shape
    ffn = weights[0].shape[1]
    y = jax.ShapeDtypeStruct((tokens, model), jnp.bfloat16)
    any_spec, vmem_spec = pl.BlockSpec(memory_space=pl.ANY), pl.BlockSpec(memory_space=pltpu.VMEM)
    widths = [width for _, width, _ in PARTS]
    back = [pltpu.VMEM((8, RING, RING, SLOTS, width), jnp.bfloat16) for width in widths]
    rows = [pltpu.VMEM((RING - 1, 8, RING, SLOTS, width), jnp.bfloat16) for width in widths]
    sums = [pltpu.VMEM((RING - 1, tokens, width), jnp.float32) for width in widths]
    dma = pltpu.SemaphoreType.DMA
    return pl.pallas_call(
        return_kernel,
        out_shape=(y, y, jax.ShapeDtypeStruct(x_b.shape, x_b.dtype)),
        in_specs=[vmem_spec] + [any_spec] * 2 + [vmem_spec] * 4 + [any_spec] * 3,
        out_specs=(vmem_spec, vmem_spec, any_spec),
        scratch_shapes=back * 2 + rows * 2 + sums * 3 + [pltpu.VMEM((tokens, model), jnp.float32)]
        + [dma((2, 3, RING)), dma((2, 3)), dma((2, 3)), dma((2, 3, 3)), dma((2, 3)), dma((2, 3, 3)), dma((3,))]
        + expert_scratch(model, ffn),
        compiler_params=pltpu.CompilerParams(collective_id=1, has_side_effects=True, vmem_limit_bytes=63 * 1024 * 1024),
        name="return_rows",
    )(ids, done_a, x_b, *metas, *residuals, *weights)[:2]


def solution(mesh):
    row_spec = P(("dp", "ep"), None)
    full_spec = P(None, None, None)
    gain_spec = P(None)
    expert_spec = P("ep", None, None)
    in_specs = (row_spec,) * 8 + (gain_spec,) + (full_spec,) * 4 + (gain_spec,) + (expert_spec,) * 3

    def device_fn(tokens_a, experts_a, slots_a, gates_a, tokens_b, experts_b, slots_b, gates_b, attn_gain, w_query, w_key, w_value, w_out, moe_gain, w_gate, w_up, w_down):
        w_gate, w_up, w_down = w_gate[0], w_up[0], w_down[0]
        ids = jnp.stack([row_ids(order) for _, _, order in PARTS])

        res_a, res_b, own_a, own_b = attention(
            tokens_a, (experts_a, slots_a, gates_a), tokens_b, (experts_b, slots_b, gates_b), attn_gain, moe_gain, w_query, w_key, w_value, w_out
        )
        weights = (w_gate, w_up, w_down)
        _, x_b, meta_a, meta_b, done_a = dispatch(own_a, own_b, ids[:, :128], weights)
        return bring_back(ids, done_a, x_b, (meta_a, meta_b), (res_a, res_b), weights)

    return jax.shard_map(device_fn, mesh=mesh, in_specs=in_specs, out_specs=(row_spec, row_spec), check_vma=False)
```

```python
import jax
import jax.numpy as jnp
from jax import lax
from jax.experimental import pallas as pl
from jax.experimental.pallas import tpu as pltpu
from jax.sharding import PartitionSpec as P

NORM_EPS = 1e-6
MASK_VALUE = -1e30
RING = 4
CORES = 2
SLOTS = 16
HEAD_DIM = 64
PARTS = (
    (0, 640, ("z", "y", "x")),
    (640, 640, ("x", "z", "y")),
    (1280, 768, ("y", "x", "z")),
)
STRIDE = {"z": 32, "y": 8, "x": 2}

def coords(index):
    return {"z": index // 32, "y": (index // 8) % RING, "x": (index // 2) % RING}, index % CORES


def peer(dim, delta, flip=0):
    me = lax.axis_index("ep")
    stride = STRIDE[dim]
    place = lax.rem(me // stride, RING)
    other = me + (lax.rem(place + delta % RING, RING) - place) * stride
    if flip:
        other = other + 1 - 2 * lax.rem(me, CORES)
    return {"ep": other}


def send(src, dst, send_sem, recv_sem, where):
    return pltpu.make_async_remote_copy(src_ref=src, dst_ref=dst, send_sem=send_sem, recv_sem=recv_sem, device_id=where, device_id_type=pl.DeviceIdType.MESH)


def drain(ref, sem):
    pltpu.make_async_copy(ref, ref, sem).wait()


def greet():
    barrier = pltpu.get_barrier_semaphore()
    count = 0
    for dim in ("x", "y", "z"):
        for delta in range(1, RING):
            for flip in range(CORES):
                pl.semaphore_signal(barrier, inc=1, device_id=peer(dim, delta, flip), device_id_type=pl.DeviceIdType.MESH)
                count += 1
    pl.semaphore_signal(barrier, inc=1, device_id=peer("x", 0, 1), device_id_type=pl.DeviceIdType.MESH)
    return barrier, count + 1


def group_view(rows, part, off3, flip, off2):
    start, width, (_, s2, s3) = PARTS[part]
    place = {s3: off3, s2: off2}
    index = tuple(place.get(dim, slice(None)) for dim in ("y", "z"))
    line = flip * RING + place["x"] if "x" in place else slice(flip * RING, (flip + 1) * RING)
    return rows.at[line, index[0], index[1], :, start : start + width]


def row_ids(order, off2):
    s1, s2, s3 = order
    pos, core = coords(lax.axis_index("ep"))
    row = lax.broadcasted_iota(jnp.int32, (128, 128), 0)
    slot, flip, off3 = row % SLOTS, (row // SLOTS) % CORES, row // (SLOTS * CORES)
    base = pos[s1] * STRIDE[s1] + lax.rem(pos[s2] + off2, RING) * STRIDE[s2] + core
    expert = base + (pos[s3] + off3) % RING * STRIDE[s3] + flip * (1 - 2 * core)
    return (expert * SLOTS + slot).astype(jnp.float32)


PAIRS = tuple((off, flip) for off in range(RING) for flip in range(CORES))


def routing_ids(meta):
    expert = meta[:, 0:128].astype(jnp.float32)
    slot = meta[:, 128:256].astype(jnp.float32)
    return jnp.where(slot >= 0, expert * SLOTS + slot, -1.0)


def rms_norm(rows_f, gain_ref):
    inv_rms = lax.rsqrt(jnp.mean(rows_f * rows_f, axis=-1, keepdims=True) + NORM_EPS)
    return rows_f * inv_rms * gain_ref[...].astype(jnp.float32).reshape(1, -1)


def attend(x_ref, gain_ref, w_refs, pool, sem, normed_t, total, last, between):
    tokens, model = x_ref.shape
    steps = w_refs[0].shape[0]

    def load(i, slot):
        for w, w_ref in enumerate(w_refs):
            pltpu.make_async_copy(w_ref.at[i], pool.at[slot * 4 + w], sem.at[slot]).start()

    normed_t[...] = rms_norm(x_ref[...].astype(jnp.float32), gain_ref).T.astype(jnp.bfloat16)
    total[...] = jnp.zeros_like(total)
    seen = lax.broadcasted_iota(jnp.int32, (tokens, tokens), 0) <= lax.broadcasted_iota(jnp.int32, (tokens, tokens), 1)

    def step(i, carry):
        slot = lax.rem(i, 2)
        if last:

            @pl.when(i + 1 < steps)
            def _():
                load(i + 1, 1 - slot)

        else:
            load(lax.rem(i + 1, steps), 1 - slot)
        drain(pool.at[pl.ds(slot * 4, 4)], sem.at[slot])
        query, keys, values = (
            jnp.dot(pool[slot * 4 + w].reshape(-1, model), normed_t[...], preferred_element_type=jnp.float32).astype(jnp.bfloat16) for w in range(3)
        )
        context = []
        for start in range(0, query.shape[0], HEAD_DIM):
            head = slice(start, start + HEAD_DIM)
            scores = lax.dot_general(keys[head], query[head], (((0,), (0,)), ((), ())), preferred_element_type=jnp.float32) * (HEAD_DIM**-0.5)
            scores = jnp.where(seen, scores, MASK_VALUE)
            weight = jnp.exp(scores - jnp.max(scores, axis=0, keepdims=True))
            prob = (weight / jnp.sum(weight, axis=0, keepdims=True)).astype(jnp.bfloat16)
            context.append(jnp.dot(values[head], prob, preferred_element_type=jnp.float32).astype(jnp.bfloat16))
        context = jnp.concatenate(context, axis=0)
        total[...] += lax.dot_general(context, pool[slot * 4 + 3].reshape(-1, model), (((0,), (0,)), ((), ())), preferred_element_type=jnp.float32)
        between(i)
        return carry

    if not last:
        load(0, 0)
    lax.fori_loop(0, steps, step, 0)


def load_weights(w_refs, held, sem):
    copies = [pltpu.make_async_copy(src, dst, sem.at[i]) for i, (src, dst) in enumerate(zip(w_refs, held))]
    for copy in copies:
        copy.start()
    return copies


def run_experts(x_ref, o_ref, held, pool, x_sem, o_sem, between):
    blocks = x_ref.shape[0]
    gate_w, up_w, down_w = held
    x_buf, o_buf = pool.at[0:2], pool.at[2:4]

    def load(b, slot):
        return pltpu.make_async_copy(x_ref.at[b], x_buf.at[slot], x_sem.at[slot])

    load(0, 0).start()

    def step(b, carry):
        slot = lax.rem(b, 2)

        @pl.when(b + 1 < blocks)
        def _():
            load(b + 1, 1 - slot).start()

        load(b, slot).wait()

        @pl.when(b >= 2)
        def _():
            drain(o_buf.at[slot], o_sem.at[slot])

        x = x_buf[slot].reshape(-1, gate_w.shape[0])
        gate_act = jnp.dot(x, gate_w[...], preferred_element_type=jnp.float32)
        up_act = jnp.dot(x, up_w[...], preferred_element_type=jnp.float32)
        hidden = (jax.nn.silu(gate_act) * up_act).astype(jnp.bfloat16)
        o_buf[slot] = jnp.dot(hidden, down_w[...], preferred_element_type=jnp.float32).astype(jnp.bfloat16).reshape(o_buf.shape[1:])
        pltpu.make_async_copy(o_buf.at[slot], o_ref.at[b], o_sem.at[slot]).start()
        between(b)
        return carry

    lax.fori_loop(0, blocks, step, 0)
    for slot in range(2):
        drain(o_buf.at[slot], o_sem.at[slot])


def expert_scratch(model, ffn):
    dma = pltpu.SemaphoreType.DMA
    return [
        pltpu.VMEM((model, ffn), jnp.bfloat16),
        pltpu.VMEM((model, ffn), jnp.bfloat16),
        pltpu.VMEM((ffn, model), jnp.bfloat16),
        dma((3,)),
        dma((2,)),
        dma((2,)),
    ]


def dispatch_kernel(*refs):
    batches = 2
    x_refs, routing_refs, gain_refs, aw_refs, w_refs = refs[0:2], (refs[2:5], refs[5:8]), refs[8:10], refs[10:14], refs[14:17]
    out_refs, meta_refs, res_refs, done_ref = refs[17:19], refs[19:21], refs[21:23], refs[23]
    scratch = refs[24:]
    planes = [scratch[3 * n : 3 + 3 * n] for n in range(batches)]
    chosen = [scratch[6 + 3 * n : 9 + 3 * n] for n in range(batches)]
    plane_recv, plane_send, row_recv, row_send, local_sem = scratch[12:17]
    own_refs, normed_t, total, ids_ref, pool, attn_sem = scratch[17:19], scratch[19], scratch[20], scratch[21], scratch[22], scratch[23]
    held, (w_sem, x_sem, o_sem) = scratch[24:27], scratch[27:]
    tokens = x_refs[0].shape[0]
    half = tokens // 2
    barrier, greetings = greet()

    def own_part(n, part):
        start, width, _ = PARTS[part]
        return own_refs[n].at[:, start : start + width]

    def attention(n, between):
        attend(x_refs[n], gain_refs[0], aw_refs, pool, attn_sem, normed_t, total, n == batches - 1, between)
        residual = (x_refs[n][...].astype(jnp.float32) + total[...]).astype(jnp.bfloat16)
        res_refs[n][...] = residual
        own_refs[n][0:tokens, :] = rms_norm(residual.astype(jnp.float32), gain_refs[1]).astype(jnp.bfloat16)
        own_refs[n][tokens : tokens + 8, :] = jnp.zeros((8, own_refs[n].shape[1]), jnp.bfloat16)
        for start, _, _ in PARTS:
            for i, ref in enumerate(routing_refs[n]):
                own_refs[n][tokens : tokens + 8, start + i * 128 : start + (i + 1) * 128] = ref[...].astype(jnp.float32).astype(jnp.bfloat16)

    def send_own(n):
        for part, (_, _, (s1, s2, _)) in enumerate(PARTS):
            plane = planes[n][part]
            for off in (1, 3, 2):
                send(own_part(n, part), plane.at[off], plane_send.at[n, part], plane_recv.at[n, part, off], peer(s1, off)).start()
            for off in (1, 3):
                send(own_part(n, part), plane.at[off * RING], plane_send.at[n, part], plane_recv.at[n, part, off * RING], peer(s2, off)).start()

    def forward(n):
        for part, (_, _, (s1, s2, _)) in enumerate(PARTS):
            plane = planes[n][part]
            for off1 in (1, 3, 2):
                drain(plane.at[off1], plane_recv.at[n, part, off1])
                for off2 in (1, 3):
                    send(plane.at[off1], plane.at[off2 * RING + off1], plane_send.at[n, part], plane_recv.at[n, part, off2 * RING + off1], peer(s2, off2)).start()

    def relay(n, off2):
        rows = slice(0, half) if off2 == 1 else slice(half, tokens + 8)
        for part, (_, _, (s1, s2, _)) in enumerate(PARTS):
            plane = planes[n][part]
            for off1 in range(RING):
                drain(plane.at[off2 * RING + off1], plane_recv.at[n, part, off2 * RING + off1])
                send(plane.at[off2 * RING + off1, rows], plane.at[2 * RING + off1, rows], plane_send.at[n, part], plane_recv.at[n, part, 2 * RING + off1], peer(s2, off2)).start()

    def select(n, part, off2, off1, block):
        width = PARTS[part][1]
        ids = ids_ref[part]
        dest = routing_ids(block[tokens : tokens + 8, 0:384])
        hit = ids == dest[0:1, :]
        for j in range(1, 8):
            hit = jnp.logical_or(hit, ids == dest[j : j + 1, :])
        onehot = jnp.where(hit, 1.0, 0.0).astype(jnp.bfloat16)
        rows = jnp.dot(onehot, block[0:tokens, :], preferred_element_type=jnp.float32).astype(jnp.bfloat16)
        chosen[n][part][:, off2, off1] = rows.reshape(8, SLOTS, width)

    def select_group(n, part, off2):
        start, width, _ = PARTS[part]
        plane = planes[n][part]
        if off2 == 0:
            meta_refs[n][part, 0] = own_refs[n][tokens : tokens + 8, start : start + 384]
            for off1 in range(1, RING):
                meta_refs[n][part, off1] = plane[off1, tokens : tokens + 8, 0:384]
            select(n, part, 0, 0, own_refs[n].at[:, start : start + width])
            first = 1
        else:
            for off1 in range(RING if off2 == 2 else 0):
                drain(plane.at[off2 * RING + off1], plane_recv.at[n, part, off2 * RING + off1])
            first = 0

        def body(off1, carry):
            select(n, part, off2, off1, plane.at[off2 * RING + off1])
            return carry

        lax.fori_loop(first, RING, body, 0)

    def send_group(n, part, off2):
        s3 = PARTS[part][2][2]
        for i in (2, 3, 6, 7, 4, 5, 1):
            off3, flip = PAIRS[i]
            send(chosen[n][part].at[i, off2], group_view(out_refs[n], part, off3, flip, off2), row_send.at[n, part], row_recv.at[n], peer(s3, off3, flip)).start()
        pltpu.make_async_copy(chosen[n][part].at[0, off2], group_view(out_refs[n], part, 0, 0, off2), local_sem.at[n, part]).start()

    late = []

    def groups(n, off2):
        for part in range(3):
            select_group(n, part, off2)
            if late:
                send_group(*late.pop())
            late.append((n, part, off2))

    def flush():
        if late:
            send_group(*late.pop())

    def under_b(i):
        @pl.when(i == 4)
        def _():
            forward(0)

        @pl.when(i == 5)
        def _():
            groups(0, 0)

        @pl.when(i == 6)
        def _():
            flush()

    attention(0, lambda i: None)
    for part, (_, _, order) in enumerate(PARTS):
        ids_ref[part] = row_ids(order, 0)
    pl.semaphore_wait(barrier, greetings)
    send_own(0)
    attention(1, under_b)
    weight_copies = load_weights(w_refs, held, w_sem)
    send_own(1)
    relay(0, 1)
    relay(0, 3)
    groups(0, 1)
    groups(0, 3)
    forward(1)
    flush()
    groups(0, 2)
    groups(1, 0)
    relay(1, 1)
    relay(1, 3)
    flush()
    for off2 in (1, 3, 2):
        groups(1, off2)
    flush()

    def rows_done(n):
        drain(out_refs[n].at[1:8], row_recv.at[n])
        for part in range(3):
            drain(chosen[n][part].at[0], local_sem.at[n, part])

    rows_done(0)
    for copy in weight_copies:
        copy.wait()
    run_experts(out_refs[0], done_ref, held, pool, x_sem, o_sem, lambda b: None)
    rows_done(1)
    for n in range(batches):
        for part in range(3):
            drain(planes[n][part].at[1:16], plane_send.at[n, part])
            drain(chosen[n][part].at[1:8], row_send.at[n, part])


def dispatch(tokens, routing, gains, attention_weights, weights):
    rows, model = tokens[0].shape
    ffn = weights[0].shape[1]
    block = (RING, RING, SLOTS, model)
    out = jax.ShapeDtypeStruct((CORES * RING,) + block, jnp.bfloat16)
    meta = jax.ShapeDtypeStruct((3, RING, 8, 384), jnp.bfloat16)
    residual = jax.ShapeDtypeStruct((rows, model), jnp.bfloat16)
    any_spec, vmem_spec = pl.BlockSpec(memory_space=pl.ANY), pl.BlockSpec(memory_space=pltpu.VMEM)
    plane = [pltpu.VMEM((RING * RING, rows + 8, width), jnp.bfloat16) for _, width, _ in PARTS]
    chosen = [pltpu.VMEM((8, RING, RING, SLOTS, width), jnp.bfloat16) for _, width, _ in PARTS]
    own = pltpu.VMEM((rows + 8, model), jnp.bfloat16)
    dma = pltpu.SemaphoreType.DMA
    return pl.pallas_call(
        dispatch_kernel,
        out_shape=(out, out, meta, meta, residual, residual, out),
        in_specs=[vmem_spec] * 10 + [any_spec] * 7,
        out_specs=(any_spec,) * 2 + (vmem_spec,) * 4 + (any_spec,),
        scratch_shapes=plane * 2
        + chosen * 2
        + [dma((2, 3, 16)), dma((2, 3)), dma((2,)), dma((2, 3)), dma((2, 3))]
        + [own, own, pltpu.VMEM((model, rows), jnp.bfloat16), pltpu.VMEM((rows, model), jnp.float32), pltpu.VMEM((3, 128, 128), jnp.float32)]
        + [pltpu.VMEM((8,) + block, jnp.bfloat16), dma((2,))]
        + expert_scratch(model, ffn),
        compiler_params=pltpu.CompilerParams(collective_id=0, has_side_effects=True, vmem_limit_bytes=63 * 1024 * 1024),
        name="dispatch_rows",
    )(*tokens, *routing[0], *routing[1], *gains, *(w.reshape((8,) + block) for w in attention_weights), *weights)


def return_kernel(*refs):
    batches = 2
    done_a, x_b, meta_refs, res_refs, w_refs = refs[0], refs[1], refs[2:4], refs[4:6], refs[6:9]
    y_refs, done_b, scratch = refs[9:11], refs[11], refs[12:]
    out_refs = (done_a, done_b)
    back = [scratch[0 + 3 * n : 3 + 3 * n] for n in range(batches)]
    rows = [scratch[6 + 3 * n : 9 + 3 * n] for n in range(batches)]
    sums, got = scratch[12:15], [scratch[15 + 3 * n : 18 + 3 * n] for n in range(batches)]
    kept = scratch[21]
    back_recv, back_send, own_sem, rows_recv, rows_send, sums_recv, sums_send = scratch[22:29]
    ids_ref, pool = scratch[29:31]
    held, (w_sem, x_sem, o_sem) = scratch[31:34], scratch[34:]
    tokens = y_refs[0].shape[0]
    barrier, greetings = greet()
    for part, (_, _, order) in enumerate(PARTS):
        for off2 in range(RING):
            ids_ref[part, off2] = row_ids(order, off2)
    pl.semaphore_wait(barrier, greetings)
    weight_copies = load_weights(w_refs, held, w_sem)

    def hand_out(n):
        for part in range(3):
            for off2 in range(RING):
                pltpu.make_async_copy(group_view(out_refs[n], part, 0, 0, off2), back[n][part].at[0, off2], own_sem.at[n, part]).start()
        for off2 in (2, 1, 3, 0):
            for i in (2, 3, 6, 7, 4, 5, 1):
                off3, flip = PAIRS[i]
                for part in range(3):
                    s3 = PARTS[part][2][2]
                    send(group_view(out_refs[n], part, off3, flip, off2), back[n][part].at[i, off2], back_send.at[n, part], back_recv.at[n, part, off2], peer(s3, -off3, flip)).start()

    def turn(n, off2):
        for part in range(3):
            s2 = PARTS[part][2][1]
            drain(back[n][part].at[1:8, off2], back_recv.at[n, part, off2])
            if off2:
                send(back[n][part].at[:, off2], rows[n][part].at[off2 - 1], rows_send.at[n, part], rows_recv.at[n, part, off2 - 1], peer(s2, -off2)).start()

    def weighted(n, part, off2, off1):
        width = PARTS[part][1]
        meta = meta_refs[n][part, off1]
        dest = routing_ids(meta)
        gates = meta[:, 256:384].astype(jnp.float32)
        ids = ids_ref[part, off2]
        weight = jnp.zeros((128, tokens), jnp.float32)
        for j in range(8):
            weight = jnp.where(ids == dest[j : j + 1, :], gates[j : j + 1, :], weight)
        block = back[n][part][:, 0, off1] if off2 == 0 else rows[n][part][off2 - 1, :, off1]
        return lax.dot_general(weight.astype(jnp.bfloat16), block.reshape(128, width), (((0,), (0,)), ((), ())), preferred_element_type=jnp.float32)

    def own_ready(n):
        for part in range(3):
            drain(back[n][part].at[0], own_sem.at[n, part])

    def add_group(n, off2, first=False, last=False):
        late = []

        def flush():
            if late:
                part, off1 = late.pop()
                s1 = PARTS[part][2][0]
                send(sums[part].at[off1 - 1], got[n][part].at[off1 - 1], sums_send.at[part], sums_recv.at[n, part, off1 - 1], peer(s1, -off1)).start()

        for part in range(3):
            start, width, _ = PARTS[part]
            if off2:
                drain(rows[n][part].at[off2 - 1], rows_recv.at[n, part, off2 - 1])
            for off1 in (2, 1, 3, 0):
                term = weighted(n, part, off2, off1)
                if off1 == 0:
                    before = res_refs[n][:, start : start + width].astype(jnp.float32) if first else kept[:, start : start + width]
                    kept[:, start : start + width] = before + term
                else:
                    sums[part][off1 - 1] = term if first else sums[part][off1 - 1] + term
                flush()
                if last and off1:
                    late.append((part, off1))

    def finish(n):
        for part in range(3):
            start, width, _ = PARTS[part]
            total = kept[:, start : start + width]
            for off1 in range(1, RING):
                drain(got[n][part].at[off1 - 1], sums_recv.at[n, part, off1 - 1])
                total = total + got[n][part][off1 - 1]
            y_refs[n][:, start : start + width] = total.astype(y_refs[n].dtype)
            drain(sums[part], sums_send.at[part])

    hand_out(0)
    for copy in weight_copies:
        copy.wait()

    def between(b):
        for when, off2 in ((1, 2), (3, 1), (5, 3), (7, 0)):

            @pl.when(b == when)
            def _():
                if off2 == 2:
                    own_ready(0)
                turn(0, off2)

    run_experts(x_b, done_b, held, pool, x_sem, o_sem, between)
    hand_out(1)
    add_group(0, 0, first=True)
    add_group(0, 2)
    add_group(0, 1)
    own_ready(1)
    turn(1, 2)
    add_group(0, 3, last=True)
    for off2 in (1, 3, 0):
        turn(1, off2)
    finish(0)
    add_group(1, 0, first=True)
    add_group(1, 2)
    add_group(1, 1)
    add_group(1, 3, last=True)
    finish(1)
    for n in range(batches):
        for part in range(3):
            drain(back[n][part].at[1:8], back_send.at[n, part])
            drain(rows[n][part], rows_send.at[n, part])


def bring_back(done_a, x_b, metas, residuals, weights):
    tokens, model = residuals[0].shape
    ffn = weights[0].shape[1]
    y = jax.ShapeDtypeStruct((tokens, model), jnp.bfloat16)
    any_spec, vmem_spec = pl.BlockSpec(memory_space=pl.ANY), pl.BlockSpec(memory_space=pltpu.VMEM)
    widths = [width for _, width, _ in PARTS]
    back = [pltpu.VMEM((8, RING, RING, SLOTS, width), jnp.bfloat16) for width in widths]
    rows = [pltpu.VMEM((RING - 1, 8, RING, SLOTS, width), jnp.bfloat16) for width in widths]
    sums = [pltpu.VMEM((RING - 1, tokens, width), jnp.float32) for width in widths]
    dma = pltpu.SemaphoreType.DMA
    return pl.pallas_call(
        return_kernel,
        out_shape=(y, y, jax.ShapeDtypeStruct(x_b.shape, x_b.dtype)),
        in_specs=[any_spec] * 2 + [vmem_spec] * 4 + [any_spec] * 3,
        out_specs=(vmem_spec, vmem_spec, any_spec),
        scratch_shapes=back * 2 + rows * 2 + sums * 3 + [pltpu.VMEM((tokens, model), jnp.float32)]
        + [dma((2, 3, RING)), dma((2, 3)), dma((2, 3)), dma((2, 3, 3)), dma((2, 3)), dma((2, 3, 3)), dma((3,))]
        + [pltpu.VMEM((3, RING, 128, 128), jnp.float32), pltpu.VMEM((4,) + x_b.shape[1:], jnp.bfloat16)]
        + expert_scratch(model, ffn),
        compiler_params=pltpu.CompilerParams(collective_id=1, has_side_effects=True, vmem_limit_bytes=63 * 1024 * 1024),
        name="return_rows",
    )(done_a, x_b, *metas, *residuals, *weights)[:2]


def solution(mesh):
    row_spec = P(("dp", "ep"), None)
    full_spec = P(None, None, None)
    gain_spec = P(None)
    expert_spec = P("ep", None, None)
    in_specs = (row_spec,) * 8 + (gain_spec,) + (full_spec,) * 4 + (gain_spec,) + (expert_spec,) * 3

    def device_fn(tokens_a, experts_a, slots_a, gates_a, tokens_b, experts_b, slots_b, gates_b, attn_gain, w_query, w_key, w_value, w_out, moe_gain, w_gate, w_up, w_down):
        weights = (w_gate[0], w_up[0], w_down[0])
        attention_weights = [jnp.transpose(w, (1, 2, 0)) for w in (w_query, w_key, w_value)] + [w_out]
        routing = [(e.T, s.T, g.T) for e, s, g in ((experts_a, slots_a, gates_a), (experts_b, slots_b, gates_b))]
        _, x_b, meta_a, meta_b, res_a, res_b, done_a = dispatch((tokens_a, tokens_b), routing, (attn_gain, moe_gain), attention_weights, weights)
        return bring_back(done_a, x_b, (meta_a, meta_b), (res_a, res_b), weights)

    return jax.shard_map(device_fn, mesh=mesh, in_specs=in_specs, out_specs=(row_spec, row_spec), check_vma=False)
```

```python
import jax
import jax.numpy as jnp
from jax import lax
from jax.experimental import pallas as pl
from jax.experimental.pallas import tpu as pltpu
from jax.sharding import PartitionSpec as P

NORM_EPS = 1e-6
MASK_VALUE = -1e30
RING = 4
CORES = 2
SLOTS = 16
HEAD_DIM = 64
PARTS = (
    (0, 640, ("z", "y", "x")),
    (640, 640, ("x", "z", "y")),
    (1280, 768, ("y", "x", "z")),
)
STRIDE = {"z": 32, "y": 8, "x": 2}

def coords(index):
    return {"z": index // 32, "y": (index // 8) % RING, "x": (index // 2) % RING}, index % CORES


def peer(dim, delta, flip=0):
    me = lax.axis_index("ep")
    stride = STRIDE[dim]
    place = lax.rem(me // stride, RING)
    other = me + (lax.rem(place + delta % RING, RING) - place) * stride
    if flip:
        other = other + 1 - 2 * lax.rem(me, CORES)
    return {"ep": other}


def send(src, dst, send_sem, recv_sem, where):
    return pltpu.make_async_remote_copy(src_ref=src, dst_ref=dst, send_sem=send_sem, recv_sem=recv_sem, device_id=where, device_id_type=pl.DeviceIdType.MESH)


def drain(ref, sem):
    pltpu.make_async_copy(ref, ref, sem).wait()


def greet():
    barrier = pltpu.get_barrier_semaphore()
    count = 0
    for dim in ("x", "y", "z"):
        for delta in range(1, RING):
            for flip in range(CORES):
                pl.semaphore_signal(barrier, inc=1, device_id=peer(dim, delta, flip), device_id_type=pl.DeviceIdType.MESH)
                count += 1
    pl.semaphore_signal(barrier, inc=1, device_id=peer("x", 0, 1), device_id_type=pl.DeviceIdType.MESH)
    return barrier, count + 1


def group_view(rows, part, off3, flip, off2):
    start, width, (_, s2, s3) = PARTS[part]
    place = {s3: off3, s2: off2}
    index = tuple(place.get(dim, slice(None)) for dim in ("y", "z"))
    line = flip * RING + place["x"] if "x" in place else slice(flip * RING, (flip + 1) * RING)
    return rows.at[line, index[0], index[1], :, start : start + width]


def row_ids(order, off2):
    s1, s2, s3 = order
    pos, core = coords(lax.axis_index("ep"))
    row = lax.broadcasted_iota(jnp.int32, (128, 128), 0)
    slot, flip, off3 = row % SLOTS, (row // SLOTS) % CORES, row // (SLOTS * CORES)
    base = pos[s1] * STRIDE[s1] + lax.rem(pos[s2] + off2, RING) * STRIDE[s2] + core
    expert = base + (pos[s3] + off3) % RING * STRIDE[s3] + flip * (1 - 2 * core)
    return (expert * SLOTS + slot).astype(jnp.float32)


PAIRS = tuple((off, flip) for off in range(RING) for flip in range(CORES))


def routing_ids(meta):
    expert = meta[:, 0:128].astype(jnp.float32)
    slot = meta[:, 128:256].astype(jnp.float32)
    return jnp.where(slot >= 0, expert * SLOTS + slot, -1.0)


def rms_norm(rows_f, gain_ref):
    inv_rms = lax.rsqrt(jnp.mean(rows_f * rows_f, axis=-1, keepdims=True) + NORM_EPS)
    return rows_f * inv_rms * gain_ref[...].astype(jnp.float32).reshape(1, -1)


def attend(x_ref, gain_ref, w_refs, pool, sem, normed_t, total, last, between):
    tokens, model = x_ref.shape
    steps = w_refs[0].shape[0]

    def load(i, slot):
        for w, w_ref in enumerate(w_refs):
            pltpu.make_async_copy(w_ref.at[i], pool.at[slot * 4 + w], sem.at[slot]).start()

    normed_t[...] = rms_norm(x_ref[...].astype(jnp.float32), gain_ref).T.astype(jnp.bfloat16)
    total[...] = jnp.zeros_like(total)
    seen = lax.broadcasted_iota(jnp.int32, (tokens, tokens), 0) <= lax.broadcasted_iota(jnp.int32, (tokens, tokens), 1)

    def step(i, carry):
        slot = lax.rem(i, 2)
        if last:

            @pl.when(i + 1 < steps)
            def _():
                load(i + 1, 1 - slot)

        else:
            load(lax.rem(i + 1, steps), 1 - slot)
        drain(pool.at[pl.ds(slot * 4, 4)], sem.at[slot])
        query, keys, values = (
            jnp.dot(pool[slot * 4 + w].reshape(-1, model), normed_t[...], preferred_element_type=jnp.float32).astype(jnp.bfloat16) for w in range(3)
        )
        context = []
        for start in range(0, query.shape[0], HEAD_DIM):
            head = slice(start, start + HEAD_DIM)
            scores = lax.dot_general(keys[head], query[head], (((0,), (0,)), ((), ())), preferred_element_type=jnp.float32) * (HEAD_DIM**-0.5)
            scores = jnp.where(seen, scores, MASK_VALUE)
            weight = jnp.exp(scores - jnp.max(scores, axis=0, keepdims=True))
            prob = (weight / jnp.sum(weight, axis=0, keepdims=True)).astype(jnp.bfloat16)
            context.append(jnp.dot(values[head], prob, preferred_element_type=jnp.float32).astype(jnp.bfloat16))
        context = jnp.concatenate(context, axis=0)
        total[...] += lax.dot_general(context, pool[slot * 4 + 3].reshape(-1, model), (((0,), (0,)), ((), ())), preferred_element_type=jnp.float32)
        between(i)
        return carry

    if not last:
        load(0, 0)
    lax.fori_loop(0, steps, step, 0)


def load_weights(w_refs, held, sem):
    copies = [pltpu.make_async_copy(src, dst, sem.at[i]) for i, (src, dst) in enumerate(zip(w_refs, held))]
    for copy in copies:
        copy.start()
    return copies


def run_experts(x_ref, o_ref, held, pool, x_sem, o_sem, between):
    blocks = x_ref.shape[0]
    gate_w, up_w, down_w = held
    x_buf, o_buf = pool.at[0:2], pool.at[2:4]

    def load(b, slot):
        return pltpu.make_async_copy(x_ref.at[b], x_buf.at[slot], x_sem.at[slot])

    load(0, 0).start()

    def step(b, carry):
        slot = lax.rem(b, 2)

        @pl.when(b + 1 < blocks)
        def _():
            load(b + 1, 1 - slot).start()

        load(b, slot).wait()

        @pl.when(b >= 2)
        def _():
            drain(o_buf.at[slot], o_sem.at[slot])

        x = x_buf[slot].reshape(-1, gate_w.shape[0])
        gate_act = jnp.dot(x, gate_w[...], preferred_element_type=jnp.float32)
        up_act = jnp.dot(x, up_w[...], preferred_element_type=jnp.float32)
        hidden = (jax.nn.silu(gate_act) * up_act).astype(jnp.bfloat16)
        o_buf[slot] = jnp.dot(hidden, down_w[...], preferred_element_type=jnp.float32).astype(jnp.bfloat16).reshape(o_buf.shape[1:])
        pltpu.make_async_copy(o_buf.at[slot], o_ref.at[b], o_sem.at[slot]).start()
        between(b)
        return carry

    lax.fori_loop(0, blocks, step, 0)
    for slot in range(2):
        drain(o_buf.at[slot], o_sem.at[slot])


def expert_scratch(model, ffn):
    dma = pltpu.SemaphoreType.DMA
    return [
        pltpu.VMEM((model, ffn), jnp.bfloat16),
        pltpu.VMEM((model, ffn), jnp.bfloat16),
        pltpu.VMEM((ffn, model), jnp.bfloat16),
        dma((3,)),
        dma((2,)),
        dma((2,)),
    ]


def dispatch_kernel(*refs):
    batches = 2
    x_refs, routing_refs, gain_refs, aw_refs, w_refs = refs[0:2], (refs[2:5], refs[5:8]), refs[8:10], refs[10:14], refs[14:17]
    out_refs, meta_refs, res_refs, done_ref = refs[17:19], refs[19:21], refs[21:23], refs[23]
    scratch = refs[24:]
    planes = [scratch[3 * n : 3 + 3 * n] for n in range(batches)]
    chosen = [scratch[6 + 3 * n : 9 + 3 * n] for n in range(batches)]
    plane_recv, plane_send, row_recv, row_send, local_sem = scratch[12:17]
    own_refs, normed_t, total, ids_ref, pool, attn_sem = scratch[17:19], scratch[19], scratch[20], scratch[21], scratch[22], scratch[23]
    held, (w_sem, x_sem, o_sem) = scratch[24:27], scratch[27:]
    tokens = x_refs[0].shape[0]
    half = tokens // 2
    barrier, greetings = greet()

    def own_part(n, part):
        start, width, _ = PARTS[part]
        return own_refs[n].at[:, start : start + width]

    def attention(n, between):
        attend(x_refs[n], gain_refs[0], aw_refs, pool, attn_sem, normed_t, total, n == batches - 1, between)
        residual = (x_refs[n][...].astype(jnp.float32) + total[...]).astype(jnp.bfloat16)
        res_refs[n][...] = residual
        own_refs[n][0:tokens, :] = rms_norm(residual.astype(jnp.float32), gain_refs[1]).astype(jnp.bfloat16)
        own_refs[n][tokens : tokens + 8, :] = jnp.zeros((8, own_refs[n].shape[1]), jnp.bfloat16)
        for start, _, _ in PARTS:
            for i, ref in enumerate(routing_refs[n]):
                own_refs[n][tokens : tokens + 8, start + i * 128 : start + (i + 1) * 128] = ref[...].astype(jnp.float32).astype(jnp.bfloat16)

    def send_own(n):
        for part, (_, _, (s1, s2, _)) in enumerate(PARTS):
            plane = planes[n][part]
            for off in (1, 3):
                send(own_part(n, part), plane.at[off], plane_send.at[n, part], plane_recv.at[n, part, off], peer(s1, off)).start()
            for off in (1, 3):
                send(own_part(n, part), plane.at[off * RING], plane_send.at[n, part], plane_recv.at[n, part, off * RING], peer(s2, off)).start()

    def forward(n, far):
        for part, (_, _, (s1, s2, _)) in enumerate(PARTS):
            plane = planes[n][part]
            for off1 in (2,) if far else (1, 3):
                drain(plane.at[off1], plane_recv.at[n, part, off1])
                if not far:
                    rows = slice(0, half) if off1 == 1 else slice(half, tokens + 8)
                    send(plane.at[off1, rows], plane.at[2, rows], plane_send.at[n, part], plane_recv.at[n, part, 2], peer(s1, off1)).start()
                for off2 in (1, 3):
                    send(plane.at[off1], plane.at[off2 * RING + off1], plane_send.at[n, part], plane_recv.at[n, part, off2 * RING + off1], peer(s2, off2)).start()

    def relay(n, off2):
        rows = slice(0, half) if off2 == 1 else slice(half, tokens + 8)
        for part, (_, _, (s1, s2, _)) in enumerate(PARTS):
            plane = planes[n][part]
            for off1 in range(RING):
                drain(plane.at[off2 * RING + off1], plane_recv.at[n, part, off2 * RING + off1])
                send(plane.at[off2 * RING + off1, rows], plane.at[2 * RING + off1, rows], plane_send.at[n, part], plane_recv.at[n, part, 2 * RING + off1], peer(s2, off2)).start()

    def select(n, part, off2, off1, block):
        width = PARTS[part][1]
        ids = ids_ref[part]
        dest = routing_ids(block[tokens : tokens + 8, 0:384])
        hit = ids == dest[0:1, :]
        for j in range(1, 8):
            hit = jnp.logical_or(hit, ids == dest[j : j + 1, :])
        onehot = jnp.where(hit, 1.0, 0.0).astype(jnp.bfloat16)
        rows = jnp.dot(onehot, block[0:tokens, :], preferred_element_type=jnp.float32).astype(jnp.bfloat16)
        chosen[n][part][:, off2, off1] = rows.reshape(8, SLOTS, width)

    def select_group(n, part, off2):
        start, width, _ = PARTS[part]
        plane = planes[n][part]
        if off2 == 0:
            meta_refs[n][part, 0] = own_refs[n][tokens : tokens + 8, start : start + 384]
            for off1 in range(1, RING):
                meta_refs[n][part, off1] = plane[off1, tokens : tokens + 8, 0:384]
            select(n, part, 0, 0, own_refs[n].at[:, start : start + width])
            first = 1
        else:
            for off1 in range(RING if off2 == 2 else 0):
                drain(plane.at[off2 * RING + off1], plane_recv.at[n, part, off2 * RING + off1])
            first = 0

        def body(off1, carry):
            select(n, part, off2, off1, plane.at[off2 * RING + off1])
            return carry

        lax.fori_loop(first, RING, body, 0)

    def send_group(n, part, off2):
        s3 = PARTS[part][2][2]
        for i in (2, 3, 6, 7, 4, 5, 1):
            off3, flip = PAIRS[i]
            send(chosen[n][part].at[i, off2], group_view(out_refs[n], part, off3, flip, off2), row_send.at[n, part], row_recv.at[n], peer(s3, off3, flip)).start()
        pltpu.make_async_copy(chosen[n][part].at[0, off2], group_view(out_refs[n], part, 0, 0, off2), local_sem.at[n, part]).start()

    late = []

    def groups(n, off2):
        for part in range(3):
            select_group(n, part, off2)
            if late:
                send_group(*late.pop())
            late.append((n, part, off2))

    def flush():
        if late:
            send_group(*late.pop())

    def under_b(i):
        @pl.when(i == 2)
        def _():
            forward(0, False)

        @pl.when(i == 6)
        def _():
            forward(0, True)

    attention(0, lambda i: None)
    for part, (_, _, order) in enumerate(PARTS):
        ids_ref[part] = row_ids(order, 0)
    pl.semaphore_wait(barrier, greetings)
    send_own(0)
    attention(1, under_b)
    weight_copies = load_weights(w_refs, held, w_sem)
    send_own(1)
    groups(0, 0)
    relay(0, 1)
    relay(0, 3)
    groups(0, 1)
    forward(1, False)
    groups(0, 3)
    forward(1, True)
    flush()
    groups(0, 2)
    groups(1, 0)
    relay(1, 1)
    relay(1, 3)
    flush()
    groups(1, 1)

    def rows_done(n):
        drain(out_refs[n].at[1:8], row_recv.at[n])
        for part in range(3):
            drain(chosen[n][part].at[0], local_sem.at[n, part])

    def under_a(b):
        @pl.when(b == 1)
        def _():
            groups(1, 3)

        @pl.when(b == 4)
        def _():
            groups(1, 2)

        @pl.when(b == 5)
        def _():
            flush()

    flush()
    rows_done(0)
    for copy in weight_copies:
        copy.wait()
    run_experts(out_refs[0], done_ref, held, pool, x_sem, o_sem, under_a)
    rows_done(1)
    for n in range(batches):
        for part in range(3):
            drain(planes[n][part].at[1:16], plane_send.at[n, part])
            drain(chosen[n][part].at[1:8], row_send.at[n, part])


def dispatch(tokens, routing, gains, attention_weights, weights):
    rows, model = tokens[0].shape
    ffn = weights[0].shape[1]
    block = (RING, RING, SLOTS, model)
    out = jax.ShapeDtypeStruct((CORES * RING,) + block, jnp.bfloat16)
    meta = jax.ShapeDtypeStruct((3, RING, 8, 384), jnp.bfloat16)
    residual = jax.ShapeDtypeStruct((rows, model), jnp.bfloat16)
    any_spec, vmem_spec = pl.BlockSpec(memory_space=pl.ANY), pl.BlockSpec(memory_space=pltpu.VMEM)
    plane = [pltpu.VMEM((RING * RING, rows + 8, width), jnp.bfloat16) for _, width, _ in PARTS]
    chosen = [pltpu.VMEM((8, RING, RING, SLOTS, width), jnp.bfloat16) for _, width, _ in PARTS]
    own = pltpu.VMEM((rows + 8, model), jnp.bfloat16)
    dma = pltpu.SemaphoreType.DMA
    return pl.pallas_call(
        dispatch_kernel,
        out_shape=(out, out, meta, meta, residual, residual, out),
        in_specs=[vmem_spec] * 10 + [any_spec] * 7,
        out_specs=(any_spec,) * 2 + (vmem_spec,) * 4 + (any_spec,),
        scratch_shapes=plane * 2
        + chosen * 2
        + [dma((2, 3, 16)), dma((2, 3)), dma((2,)), dma((2, 3)), dma((2, 3))]
        + [own, own, pltpu.VMEM((model, rows), jnp.bfloat16), pltpu.VMEM((rows, model), jnp.float32), pltpu.VMEM((3, 128, 128), jnp.float32)]
        + [pltpu.VMEM((8,) + block, jnp.bfloat16), dma((2,))]
        + expert_scratch(model, ffn),
        compiler_params=pltpu.CompilerParams(collective_id=0, has_side_effects=True, vmem_limit_bytes=63 * 1024 * 1024),
        name="dispatch_rows",
    )(*tokens, *routing[0], *routing[1], *gains, *(w.reshape((8,) + block) for w in attention_weights), *weights)


def return_kernel(*refs):
    batches = 2
    done_a, x_b, meta_refs, res_refs, w_refs = refs[0], refs[1], refs[2:4], refs[4:6], refs[6:9]
    y_refs, done_b, scratch = refs[9:11], refs[11], refs[12:]
    out_refs = (done_a, done_b)
    back = [scratch[0 + 3 * n : 3 + 3 * n] for n in range(batches)]
    rows = [scratch[6 + 3 * n : 9 + 3 * n] for n in range(batches)]
    sums, got = scratch[12:15], [scratch[15 + 3 * n : 18 + 3 * n] for n in range(batches)]
    kept = scratch[21]
    back_recv, back_send, own_sem, rows_recv, rows_send, sums_recv, sums_send = scratch[22:29]
    ids_ref, pool = scratch[29:31]
    held, (w_sem, x_sem, o_sem) = scratch[31:34], scratch[34:]
    tokens = y_refs[0].shape[0]
    barrier, greetings = greet()
    for part, (_, _, order) in enumerate(PARTS):
        for off2 in range(RING):
            ids_ref[part, off2] = row_ids(order, off2)
    pl.semaphore_wait(barrier, greetings)
    weight_copies = load_weights(w_refs, held, w_sem)

    def hand_out(n):
        for part in range(3):
            for off2 in range(RING):
                pltpu.make_async_copy(group_view(out_refs[n], part, 0, 0, off2), back[n][part].at[0, off2], own_sem.at[n, part]).start()
        for off2 in (2, 1, 3, 0):
            for i in (2, 3, 6, 7, 4, 5, 1):
                off3, flip = PAIRS[i]
                for part in range(3):
                    s3 = PARTS[part][2][2]
                    send(group_view(out_refs[n], part, off3, flip, off2), back[n][part].at[i, off2], back_send.at[n, part], back_recv.at[n, part, off2], peer(s3, -off3, flip)).start()

    def turn(n, off2):
        for part in range(3):
            s2 = PARTS[part][2][1]
            drain(back[n][part].at[1:8, off2], back_recv.at[n, part, off2])
            if off2:
                send(back[n][part].at[:, off2], rows[n][part].at[off2 - 1], rows_send.at[n, part], rows_recv.at[n, part, off2 - 1], peer(s2, -off2)).start()

    def weighted(n, part, off2, off1):
        width = PARTS[part][1]
        meta = meta_refs[n][part, off1]
        dest = routing_ids(meta)
        gates = meta[:, 256:384].astype(jnp.float32)
        ids = ids_ref[part, off2]
        weight = jnp.zeros((128, tokens), jnp.float32)
        for j in range(8):
            weight = jnp.where(ids == dest[j : j + 1, :], gates[j : j + 1, :], weight)
        block = back[n][part][:, 0, off1] if off2 == 0 else rows[n][part][off2 - 1, :, off1]
        return lax.dot_general(weight.astype(jnp.bfloat16), block.reshape(128, width), (((0,), (0,)), ((), ())), preferred_element_type=jnp.float32)

    def own_ready(n):
        for part in range(3):
            drain(back[n][part].at[0], own_sem.at[n, part])

    def add_group(n, off2, first=False, last=False):
        late = []

        def flush():
            if late:
                part = late.pop()
                s1 = PARTS[part][2][0]
                for rows_half, off in ((slice(0, tokens // 2), -1), (slice(tokens // 2, tokens), 1)):
                    send(sums[part].at[1, rows_half], got[n][part].at[2, rows_half], sums_send.at[part], sums_recv.at[n, part, 2], peer(s1, off)).start()

        for part in range(3):
            start, width, _ = PARTS[part]
            if off2:
                drain(rows[n][part].at[off2 - 1], rows_recv.at[n, part, off2 - 1])
            for off1 in (2, 1, 3, 0):
                term = weighted(n, part, off2, off1)
                if off1 == 0:
                    before = res_refs[n][:, start : start + width].astype(jnp.float32) if first else kept[:, start : start + width]
                    kept[:, start : start + width] = before + term
                else:
                    sums[part][off1 - 1] = term if first else sums[part][off1 - 1] + term
                flush()
                if last and off1 == 2:
                    late.append(part)

    def pass_on(n):
        def out(part):
            s1 = PARTS[part][2][0]
            for off1, place in ((1, 0), (3, 1)):
                send(sums[part].at[off1 - 1], got[n][part].at[place], sums_send.at[part], sums_recv.at[n, part, place], peer(s1, -off1)).start()

        middle = tokens // 2
        for part in range(3):
            drain(got[n][part].at[2], sums_recv.at[n, part, 2])
            sums[part][0, 0:middle] = sums[part][0, 0:middle] + got[n][part][2, 0:middle]
            sums[part][2, middle:] = sums[part][2, middle:] + got[n][part][2, middle:]
            if part:
                out(part - 1)
        out(2)

    def finish(n):
        for part in range(3):
            start, width, _ = PARTS[part]
            total = kept[:, start : start + width]
            for place in range(2):
                drain(got[n][part].at[place], sums_recv.at[n, part, place])
                total = total + got[n][part][place]
            y_refs[n][:, start : start + width] = total.astype(y_refs[n].dtype)
            drain(sums[part], sums_send.at[part])

    hand_out(0)
    for copy in weight_copies:
        copy.wait()

    def between(b):
        for when, off2 in ((2, 2), (4, 1), (6, 3)):

            @pl.when(b == when)
            def _():
                if off2 == 2:
                    own_ready(0)
                turn(0, off2)

    run_experts(x_b, done_b, held, pool, x_sem, o_sem, between)
    hand_out(1)
    turn(0, 0)
    add_group(0, 0, first=True)
    add_group(0, 2)
    add_group(0, 1)
    own_ready(1)
    turn(1, 2)
    add_group(0, 3, last=True)
    turn(1, 1)
    pass_on(0)
    turn(1, 3)
    turn(1, 0)
    finish(0)
    add_group(1, 0, first=True)
    add_group(1, 2)
    add_group(1, 1)
    add_group(1, 3, last=True)
    pass_on(1)
    finish(1)
    for n in range(batches):
        for part in range(3):
            drain(back[n][part].at[1:8], back_send.at[n, part])
            drain(rows[n][part], rows_send.at[n, part])


def bring_back(done_a, x_b, metas, residuals, weights):
    tokens, model = residuals[0].shape
    ffn = weights[0].shape[1]
    y = jax.ShapeDtypeStruct((tokens, model), jnp.bfloat16)
    any_spec, vmem_spec = pl.BlockSpec(memory_space=pl.ANY), pl.BlockSpec(memory_space=pltpu.VMEM)
    widths = [width for _, width, _ in PARTS]
    back = [pltpu.VMEM((8, RING, RING, SLOTS, width), jnp.bfloat16) for width in widths]
    rows = [pltpu.VMEM((RING - 1, 8, RING, SLOTS, width), jnp.bfloat16) for width in widths]
    sums = [pltpu.VMEM((RING - 1, tokens, width), jnp.float32) for width in widths]
    dma = pltpu.SemaphoreType.DMA
    return pl.pallas_call(
        return_kernel,
        out_shape=(y, y, jax.ShapeDtypeStruct(x_b.shape, x_b.dtype)),
        in_specs=[any_spec] * 2 + [vmem_spec] * 4 + [any_spec] * 3,
        out_specs=(vmem_spec, vmem_spec, any_spec),
        scratch_shapes=back * 2 + rows * 2 + sums * 3 + [pltpu.VMEM((tokens, model), jnp.float32)]
        + [dma((2, 3, RING)), dma((2, 3)), dma((2, 3)), dma((2, 3, 3)), dma((2, 3)), dma((2, 3, 3)), dma((3,))]
        + [pltpu.VMEM((3, RING, 128, 128), jnp.float32), pltpu.VMEM((4,) + x_b.shape[1:], jnp.bfloat16)]
        + expert_scratch(model, ffn),
        compiler_params=pltpu.CompilerParams(collective_id=1, has_side_effects=True, vmem_limit_bytes=63 * 1024 * 1024),
        name="return_rows",
    )(done_a, x_b, *metas, *residuals, *weights)[:2]


def solution(mesh):
    row_spec = P(("dp", "ep"), None)
    full_spec = P(None, None, None)
    gain_spec = P(None)
    expert_spec = P("ep", None, None)
    in_specs = (row_spec,) * 8 + (gain_spec,) + (full_spec,) * 4 + (gain_spec,) + (expert_spec,) * 3

    def device_fn(tokens_a, experts_a, slots_a, gates_a, tokens_b, experts_b, slots_b, gates_b, attn_gain, w_query, w_key, w_value, w_out, moe_gain, w_gate, w_up, w_down):
        weights = (w_gate[0], w_up[0], w_down[0])
        attention_weights = [jnp.transpose(w, (1, 2, 0)) for w in (w_query, w_key, w_value)] + [w_out]
        routing = [(e.T, s.T, g.T) for e, s, g in ((experts_a, slots_a, gates_a), (experts_b, slots_b, gates_b))]
        _, x_b, meta_a, meta_b, res_a, res_b, done_a = dispatch((tokens_a, tokens_b), routing, (attn_gain, moe_gain), attention_weights, weights)
        return bring_back(done_a, x_b, (meta_a, meta_b), (res_a, res_b), weights)

    return jax.shard_map(device_fn, mesh=mesh, in_specs=in_specs, out_specs=(row_spec, row_spec), check_vma=False)
```

```python
import jax
import jax.numpy as jnp
from jax import lax
from jax.experimental import pallas as pl
from jax.experimental.pallas import tpu as pltpu
from jax.sharding import PartitionSpec as P

NORM_EPS = 1e-6
MASK_VALUE = -1e30
RING = 4
CORES = 2
SLOTS = 16
HEAD_DIM = 64
ORDERS = (("z", "y", "x"), ("x", "z", "y"), ("y", "x", "z"))
PARTS = (
    ((0, 640, ORDERS[0]), (640, 640, ORDERS[1]), (1280, 768, ORDERS[2])),
    ((0, 768, ORDERS[0]), (768, 640, ORDERS[1]), (1408, 640, ORDERS[2])),
)
STRIDE = {"z": 32, "y": 8, "x": 2}

def coords(index):
    return {"z": index // 32, "y": (index // 8) % RING, "x": (index // 2) % RING}, index % CORES


def peer(dim, delta, flip=0):
    me = lax.axis_index("ep")
    stride = STRIDE[dim]
    place = lax.rem(me // stride, RING)
    other = me + (lax.rem(place + delta % RING, RING) - place) * stride
    if flip:
        other = other + 1 - 2 * lax.rem(me, CORES)
    return {"ep": other}


def send(src, dst, send_sem, recv_sem, where):
    return pltpu.make_async_remote_copy(src_ref=src, dst_ref=dst, send_sem=send_sem, recv_sem=recv_sem, device_id=where, device_id_type=pl.DeviceIdType.MESH)


def drain(ref, sem):
    pltpu.make_async_copy(ref, ref, sem).wait()


def greet():
    barrier = pltpu.get_barrier_semaphore()
    count = 0
    for dim in ("x", "y", "z"):
        for delta in range(1, RING):
            for flip in range(CORES):
                pl.semaphore_signal(barrier, inc=1, device_id=peer(dim, delta, flip), device_id_type=pl.DeviceIdType.MESH)
                count += 1
    pl.semaphore_signal(barrier, inc=1, device_id=peer("x", 0, 1), device_id_type=pl.DeviceIdType.MESH)
    return barrier, count + 1


def group_view(rows, n, part, off3, flip, off2):
    start, width, (_, s2, s3) = PARTS[n][part]
    place = {s3: off3, s2: off2}
    index = tuple(place.get(dim, slice(None)) for dim in ("y", "z"))
    line = flip * RING + place["x"] if "x" in place else slice(flip * RING, (flip + 1) * RING)
    return rows.at[line, index[0], index[1], :, start : start + width]


def row_ids(order, off2):
    s1, s2, s3 = order
    pos, core = coords(lax.axis_index("ep"))
    row = lax.broadcasted_iota(jnp.int32, (128, 128), 0)
    slot, flip, off3 = row % SLOTS, (row // SLOTS) % CORES, row // (SLOTS * CORES)
    base = pos[s1] * STRIDE[s1] + lax.rem(pos[s2] + off2, RING) * STRIDE[s2] + core
    expert = base + (pos[s3] + off3) % RING * STRIDE[s3] + flip * (1 - 2 * core)
    return (expert * SLOTS + slot).astype(jnp.float32)


PAIRS = tuple((off, flip) for off in range(RING) for flip in range(CORES))


def routing_ids(meta):
    expert = meta[:, 0:128].astype(jnp.float32)
    slot = meta[:, 128:256].astype(jnp.float32)
    return jnp.where(slot >= 0, expert * SLOTS + slot, -1.0)


def rms_norm(rows_f, gain_ref):
    inv_rms = lax.rsqrt(jnp.mean(rows_f * rows_f, axis=-1, keepdims=True) + NORM_EPS)
    return rows_f * inv_rms * gain_ref[...].astype(jnp.float32).reshape(1, -1)


def attend(x_ref, gain_ref, w_refs, pool, sem, normed_t, total, last, between):
    tokens, model = x_ref.shape
    steps = w_refs[0].shape[0]

    def load(i, slot):
        for w, w_ref in enumerate(w_refs):
            pltpu.make_async_copy(w_ref.at[i], pool.at[slot * 4 + w], sem.at[slot]).start()

    normed_t[...] = rms_norm(x_ref[...].astype(jnp.float32), gain_ref).T.astype(jnp.bfloat16)
    total[...] = jnp.zeros_like(total)
    seen = lax.broadcasted_iota(jnp.int32, (tokens, tokens), 0) <= lax.broadcasted_iota(jnp.int32, (tokens, tokens), 1)

    def step(i, carry):
        slot = lax.rem(i, 2)
        if last:

            @pl.when(i + 1 < steps)
            def _():
                load(i + 1, 1 - slot)

        else:
            load(lax.rem(i + 1, steps), 1 - slot)
        drain(pool.at[pl.ds(slot * 4, 4)], sem.at[slot])
        query, keys, values = (
            jnp.dot(pool[slot * 4 + w].reshape(-1, model), normed_t[...], preferred_element_type=jnp.float32).astype(jnp.bfloat16) for w in range(3)
        )
        context = []
        for start in range(0, query.shape[0], HEAD_DIM):
            head = slice(start, start + HEAD_DIM)
            scores = lax.dot_general(keys[head], query[head], (((0,), (0,)), ((), ())), preferred_element_type=jnp.float32) * (HEAD_DIM**-0.5)
            scores = jnp.where(seen, scores, MASK_VALUE)
            weight = jnp.exp(scores - jnp.max(scores, axis=0, keepdims=True))
            prob = (weight / jnp.sum(weight, axis=0, keepdims=True)).astype(jnp.bfloat16)
            context.append(jnp.dot(values[head], prob, preferred_element_type=jnp.float32).astype(jnp.bfloat16))
        context = jnp.concatenate(context, axis=0)
        total[...] += lax.dot_general(context, pool[slot * 4 + 3].reshape(-1, model), (((0,), (0,)), ((), ())), preferred_element_type=jnp.float32)
        between(i)
        return carry

    if not last:
        load(0, 0)
    lax.fori_loop(0, steps, step, 0)


def load_weights(w_refs, held, sem):
    copies = [pltpu.make_async_copy(src, dst, sem.at[i]) for i, (src, dst) in enumerate(zip(w_refs, held))]
    for copy in copies:
        copy.start()
    return copies


def run_experts(x_ref, o_ref, held, pool, x_sem, o_sem, between):
    blocks = x_ref.shape[0]
    gate_w, up_w, down_w = held
    x_buf, o_buf = pool.at[0:2], pool.at[2:4]

    def load(b, slot):
        return pltpu.make_async_copy(x_ref.at[b], x_buf.at[slot], x_sem.at[slot])

    load(0, 0).start()

    def step(b, carry):
        slot = lax.rem(b, 2)

        @pl.when(b + 1 < blocks)
        def _():
            load(b + 1, 1 - slot).start()

        load(b, slot).wait()

        @pl.when(b >= 2)
        def _():
            drain(o_buf.at[slot], o_sem.at[slot])

        x = x_buf[slot].reshape(-1, gate_w.shape[0])
        gate_act = jnp.dot(x, gate_w[...], preferred_element_type=jnp.float32)
        up_act = jnp.dot(x, up_w[...], preferred_element_type=jnp.float32)
        hidden = (jax.nn.silu(gate_act) * up_act).astype(jnp.bfloat16)
        o_buf[slot] = jnp.dot(hidden, down_w[...], preferred_element_type=jnp.float32).astype(jnp.bfloat16).reshape(o_buf.shape[1:])
        pltpu.make_async_copy(o_buf.at[slot], o_ref.at[b], o_sem.at[slot]).start()
        between(b)
        return carry

    lax.fori_loop(0, blocks, step, 0)
    for slot in range(2):
        drain(o_buf.at[slot], o_sem.at[slot])


def expert_scratch(model, ffn):
    dma = pltpu.SemaphoreType.DMA
    return [
        pltpu.VMEM((model, ffn), jnp.bfloat16),
        pltpu.VMEM((model, ffn), jnp.bfloat16),
        pltpu.VMEM((ffn, model), jnp.bfloat16),
        dma((3,)),
        dma((2,)),
        dma((2,)),
    ]


def dispatch_kernel(*refs):
    batches = 2
    x_refs, routing_refs, gain_refs, aw_refs, w_refs = refs[0:2], (refs[2:5], refs[5:8]), refs[8:10], refs[10:14], refs[14:17]
    out_refs, meta_refs, res_refs, done_ref = refs[17:19], refs[19:21], refs[21:23], refs[23]
    scratch = refs[24:]
    planes = [scratch[3 * n : 3 + 3 * n] for n in range(batches)]
    chosen = [scratch[6 + 3 * n : 9 + 3 * n] for n in range(batches)]
    plane_recv, plane_send, row_recv, row_send, local_sem = scratch[12:17]
    own_refs, normed_t, total, ids_ref, pool, attn_sem = scratch[17:19], scratch[19], scratch[20], scratch[21], scratch[22], scratch[23]
    held, (w_sem, x_sem, o_sem) = scratch[24:27], scratch[27:]
    tokens = x_refs[0].shape[0]
    half = tokens // 2
    barrier, greetings = greet()

    def own_part(n, part):
        start, width, _ = PARTS[n][part]
        return own_refs[n].at[:, start : start + width]

    def attention(n, between):
        attend(x_refs[n], gain_refs[0], aw_refs, pool, attn_sem, normed_t, total, n == batches - 1, between)
        residual = (x_refs[n][...].astype(jnp.float32) + total[...]).astype(jnp.bfloat16)
        res_refs[n][...] = residual
        own_refs[n][0:tokens, :] = rms_norm(residual.astype(jnp.float32), gain_refs[1]).astype(jnp.bfloat16)
        own_refs[n][tokens : tokens + 8, :] = jnp.zeros((8, own_refs[n].shape[1]), jnp.bfloat16)
        for start, _, _ in PARTS[n]:
            for i, ref in enumerate(routing_refs[n]):
                own_refs[n][tokens : tokens + 8, start + i * 128 : start + (i + 1) * 128] = ref[...].astype(jnp.float32).astype(jnp.bfloat16)

    def send_own(n):
        for part, (_, _, (s1, s2, _)) in enumerate(PARTS[n]):
            plane = planes[n][part]
            for off in (1, 3):
                send(own_part(n, part), plane.at[off], plane_send.at[n, part], plane_recv.at[n, part, off], peer(s1, off)).start()
            for off in (1, 3):
                send(own_part(n, part), plane.at[off * RING], plane_send.at[n, part], plane_recv.at[n, part, off * RING], peer(s2, off)).start()

    def forward(n, far):
        for part, (_, _, (s1, s2, _)) in enumerate(PARTS[n]):
            plane = planes[n][part]
            for off1 in (2,) if far else (1, 3):
                drain(plane.at[off1], plane_recv.at[n, part, off1])
                if not far:
                    rows = slice(0, half) if off1 == 1 else slice(half, tokens + 8)
                    send(plane.at[off1, rows], plane.at[2, rows], plane_send.at[n, part], plane_recv.at[n, part, 2], peer(s1, off1)).start()
                for off2 in (1, 3):
                    send(plane.at[off1], plane.at[off2 * RING + off1], plane_send.at[n, part], plane_recv.at[n, part, off2 * RING + off1], peer(s2, off2)).start()

    def relay(n, off2):
        rows = slice(0, half) if off2 == 1 else slice(half, tokens + 8)
        for part, (_, _, (s1, s2, _)) in enumerate(PARTS[n]):
            plane = planes[n][part]
            for off1 in range(RING):
                drain(plane.at[off2 * RING + off1], plane_recv.at[n, part, off2 * RING + off1])
                send(plane.at[off2 * RING + off1, rows], plane.at[2 * RING + off1, rows], plane_send.at[n, part], plane_recv.at[n, part, 2 * RING + off1], peer(s2, off2)).start()

    def select(n, part, off2, off1, block):
        width = PARTS[n][part][1]
        ids = ids_ref[part]
        dest = routing_ids(block[tokens : tokens + 8, 0:384])
        hit = ids == dest[0:1, :]
        for j in range(1, 8):
            hit = jnp.logical_or(hit, ids == dest[j : j + 1, :])
        onehot = jnp.where(hit, 1.0, 0.0).astype(jnp.bfloat16)
        rows = jnp.dot(onehot, block[0:tokens, :], preferred_element_type=jnp.float32).astype(jnp.bfloat16)
        chosen[n][part][:, off2, off1] = rows.reshape(8, SLOTS, width)

    def select_group(n, part, off2):
        start, width, _ = PARTS[n][part]
        plane = planes[n][part]
        if off2 == 0:
            meta_refs[n][part, 0] = own_refs[n][tokens : tokens + 8, start : start + 384]
            for off1 in range(1, RING):
                meta_refs[n][part, off1] = plane[off1, tokens : tokens + 8, 0:384]
            select(n, part, 0, 0, own_refs[n].at[:, start : start + width])
            first = 1
        else:
            for off1 in range(RING if off2 == 2 else 0):
                drain(plane.at[off2 * RING + off1], plane_recv.at[n, part, off2 * RING + off1])
            first = 0

        def body(off1, carry):
            select(n, part, off2, off1, plane.at[off2 * RING + off1])
            return carry

        lax.fori_loop(first, RING, body, 0)

    def send_group(n, part, off2):
        s3 = ORDERS[part][2]
        for i in (2, 3, 6, 7, 4, 5, 1):
            off3, flip = PAIRS[i]
            send(chosen[n][part].at[i, off2], group_view(out_refs[n], n, part, off3, flip, off2), row_send.at[n, part], row_recv.at[n], peer(s3, off3, flip)).start()
        pltpu.make_async_copy(chosen[n][part].at[0, off2], group_view(out_refs[n], n, part, 0, 0, off2), local_sem.at[n, part]).start()

    late = []

    def groups(n, off2):
        for part in range(3):
            select_group(n, part, off2)
            if late:
                send_group(*late.pop())
            late.append((n, part, off2))

    def flush():
        if late:
            send_group(*late.pop())

    def under_b(i):
        @pl.when(i == 2)
        def _():
            forward(0, False)

        @pl.when(i == 6)
        def _():
            forward(0, True)

    attention(0, lambda i: None)
    for part, order in enumerate(ORDERS):
        ids_ref[part] = row_ids(order, 0)
    pl.semaphore_wait(barrier, greetings)
    send_own(0)
    attention(1, under_b)
    weight_copies = load_weights(w_refs, held, w_sem)
    send_own(1)
    groups(0, 0)
    relay(0, 1)
    relay(0, 3)
    groups(0, 1)
    forward(1, False)
    groups(0, 3)
    forward(1, True)
    flush()
    groups(0, 2)
    groups(1, 0)
    relay(1, 1)
    relay(1, 3)
    flush()
    groups(1, 1)

    def rows_done(n):
        drain(out_refs[n].at[1:8], row_recv.at[n])
        for part in range(3):
            drain(chosen[n][part].at[0], local_sem.at[n, part])

    def under_a(b):
        @pl.when(b == 1)
        def _():
            groups(1, 3)

        @pl.when(b == 4)
        def _():
            groups(1, 2)

        @pl.when(b == 5)
        def _():
            flush()

    flush()
    rows_done(0)
    for copy in weight_copies:
        copy.wait()
    run_experts(out_refs[0], done_ref, held, pool, x_sem, o_sem, under_a)
    rows_done(1)
    for n in range(batches):
        for part in range(3):
            drain(planes[n][part].at[1:16], plane_send.at[n, part])
            drain(chosen[n][part].at[1:8], row_send.at[n, part])


def dispatch(tokens, routing, gains, attention_weights, weights):
    rows, model = tokens[0].shape
    ffn = weights[0].shape[1]
    block = (RING, RING, SLOTS, model)
    out = jax.ShapeDtypeStruct((CORES * RING,) + block, jnp.bfloat16)
    meta = jax.ShapeDtypeStruct((3, RING, 8, 384), jnp.bfloat16)
    residual = jax.ShapeDtypeStruct((rows, model), jnp.bfloat16)
    any_spec, vmem_spec = pl.BlockSpec(memory_space=pl.ANY), pl.BlockSpec(memory_space=pltpu.VMEM)
    widths = [width for parts in PARTS for _, width, _ in parts]
    plane = [pltpu.VMEM((RING * RING, rows + 8, width), jnp.bfloat16) for width in widths]
    chosen = [pltpu.VMEM((8, RING, RING, SLOTS, width), jnp.bfloat16) for width in widths]
    own = pltpu.VMEM((rows + 8, model), jnp.bfloat16)
    dma = pltpu.SemaphoreType.DMA
    return pl.pallas_call(
        dispatch_kernel,
        out_shape=(out, out, meta, meta, residual, residual, out),
        in_specs=[vmem_spec] * 10 + [any_spec] * 7,
        out_specs=(any_spec,) * 2 + (vmem_spec,) * 4 + (any_spec,),
        scratch_shapes=plane
        + chosen
        + [dma((2, 3, 16)), dma((2, 3)), dma((2,)), dma((2, 3)), dma((2, 3))]
        + [own, own, pltpu.VMEM((model, rows), jnp.bfloat16), pltpu.VMEM((rows, model), jnp.float32), pltpu.VMEM((3, 128, 128), jnp.float32)]
        + [pltpu.VMEM((8,) + block, jnp.bfloat16), dma((2,))]
        + expert_scratch(model, ffn),
        compiler_params=pltpu.CompilerParams(collective_id=0, has_side_effects=True, vmem_limit_bytes=63 * 1024 * 1024),
        name="dispatch_rows",
    )(*tokens, *routing[0], *routing[1], *gains, *(w.reshape((8,) + block) for w in attention_weights), *weights)


def return_kernel(*refs):
    batches = 2
    done_a, x_b, meta_refs, res_refs, w_refs = refs[0], refs[1], refs[2:4], refs[4:6], refs[6:9]
    y_refs, done_b, scratch = refs[9:11], refs[11], refs[12:]
    out_refs = (done_a, done_b)
    back = [scratch[0 + 3 * n : 3 + 3 * n] for n in range(batches)]
    rows = [scratch[6 + 3 * n : 9 + 3 * n] for n in range(batches)]
    sums = (scratch[12:15], scratch[12:15][::-1])
    got = [scratch[15 + 3 * n : 18 + 3 * n] for n in range(batches)]
    kept = scratch[21]
    back_recv, back_send, own_sem, rows_recv, rows_send, sums_recv, sums_send = scratch[22:29]
    ids_ref, pool = scratch[29:31]
    held, (w_sem, x_sem, o_sem) = scratch[31:34], scratch[34:]
    tokens = y_refs[0].shape[0]
    barrier, greetings = greet()
    for part, order in enumerate(ORDERS):
        for off2 in range(RING):
            ids_ref[part, off2] = row_ids(order, off2)
    pl.semaphore_wait(barrier, greetings)
    weight_copies = load_weights(w_refs, held, w_sem)

    def hand_out(n):
        for part in range(3):
            for off2 in range(RING):
                pltpu.make_async_copy(group_view(out_refs[n], n, part, 0, 0, off2), back[n][part].at[0, off2], own_sem.at[n, part]).start()
        for off2 in (2, 1, 3, 0):
            for i in (2, 3, 6, 7, 4, 5, 1):
                off3, flip = PAIRS[i]
                for part in range(3):
                    s3 = ORDERS[part][2]
                    send(group_view(out_refs[n], n, part, off3, flip, off2), back[n][part].at[i, off2], back_send.at[n, part], back_recv.at[n, part, off2], peer(s3, -off3, flip)).start()

    def turn(n, off2):
        for part in range(3):
            s2 = ORDERS[part][1]
            drain(back[n][part].at[1:8, off2], back_recv.at[n, part, off2])
            if off2:
                send(back[n][part].at[:, off2], rows[n][part].at[off2 - 1], rows_send.at[n, part], rows_recv.at[n, part, off2 - 1], peer(s2, -off2)).start()

    def weighted(n, part, off2, off1):
        width = PARTS[n][part][1]
        meta = meta_refs[n][part, off1]
        dest = routing_ids(meta)
        gates = meta[:, 256:384].astype(jnp.float32)
        ids = ids_ref[part, off2]
        weight = jnp.zeros((128, tokens), jnp.float32)
        for j in range(8):
            weight = jnp.where(ids == dest[j : j + 1, :], gates[j : j + 1, :], weight)
        block = back[n][part][:, 0, off1] if off2 == 0 else rows[n][part][off2 - 1, :, off1]
        return lax.dot_general(weight.astype(jnp.bfloat16), block.reshape(128, width), (((0,), (0,)), ((), ())), preferred_element_type=jnp.float32)

    def own_ready(n):
        for part in range(3):
            drain(back[n][part].at[0], own_sem.at[n, part])

    def add_group(n, off2, first=False, last=False):
        late = []

        def flush():
            if late:
                part = late.pop()
                s1 = ORDERS[part][0]
                for rows_half, off in ((slice(0, tokens // 2), -1), (slice(tokens // 2, tokens), 1)):
                    send(sums[n][part].at[1, rows_half], got[n][part].at[2, rows_half], sums_send.at[part], sums_recv.at[n, part, 2], peer(s1, off)).start()

        for part in range(3):
            start, width, _ = PARTS[n][part]
            if off2:
                drain(rows[n][part].at[off2 - 1], rows_recv.at[n, part, off2 - 1])
            for off1 in (2, 1, 3, 0):
                term = weighted(n, part, off2, off1)
                if off1 == 0:
                    before = res_refs[n][:, start : start + width].astype(jnp.float32) if first else kept[:, start : start + width]
                    kept[:, start : start + width] = before + term
                else:
                    sums[n][part][off1 - 1] = term if first else sums[n][part][off1 - 1] + term
                flush()
                if last and off1 == 2:
                    late.append(part)

    def pass_on(n):
        def out(part):
            s1 = ORDERS[part][0]
            for off1, place in ((1, 0), (3, 1)):
                send(sums[n][part].at[off1 - 1], got[n][part].at[place], sums_send.at[part], sums_recv.at[n, part, place], peer(s1, -off1)).start()

        middle = tokens // 2
        for part in range(3):
            drain(got[n][part].at[2], sums_recv.at[n, part, 2])
            sums[n][part][0, 0:middle] = sums[n][part][0, 0:middle] + got[n][part][2, 0:middle]
            sums[n][part][2, middle:] = sums[n][part][2, middle:] + got[n][part][2, middle:]
            if part:
                out(part - 1)
        out(2)

    def finish(n):
        for part in range(3):
            start, width, _ = PARTS[n][part]
            total = kept[:, start : start + width]
            for place in range(2):
                drain(got[n][part].at[place], sums_recv.at[n, part, place])
                total = total + got[n][part][place]
            y_refs[n][:, start : start + width] = total.astype(y_refs[n].dtype)
            drain(sums[n][part], sums_send.at[part])

    hand_out(0)
    for copy in weight_copies:
        copy.wait()

    def between(b):
        for when, off2 in ((2, 2), (4, 1), (6, 3)):

            @pl.when(b == when)
            def _():
                if off2 == 2:
                    own_ready(0)
                turn(0, off2)

    run_experts(x_b, done_b, held, pool, x_sem, o_sem, between)
    hand_out(1)
    turn(0, 0)
    add_group(0, 0, first=True)
    add_group(0, 2)
    add_group(0, 1)
    own_ready(1)
    turn(1, 2)
    add_group(0, 3, last=True)
    turn(1, 1)
    pass_on(0)
    turn(1, 3)
    turn(1, 0)
    finish(0)
    add_group(1, 0, first=True)
    add_group(1, 2)
    add_group(1, 1)
    add_group(1, 3, last=True)
    pass_on(1)
    finish(1)
    for n in range(batches):
        for part in range(3):
            drain(back[n][part].at[1:8], back_send.at[n, part])
            drain(rows[n][part], rows_send.at[n, part])


def bring_back(done_a, x_b, metas, residuals, weights):
    tokens, model = residuals[0].shape
    ffn = weights[0].shape[1]
    y = jax.ShapeDtypeStruct((tokens, model), jnp.bfloat16)
    any_spec, vmem_spec = pl.BlockSpec(memory_space=pl.ANY), pl.BlockSpec(memory_space=pltpu.VMEM)
    widths = [width for parts in PARTS for _, width, _ in parts]
    back = [pltpu.VMEM((8, RING, RING, SLOTS, width), jnp.bfloat16) for width in widths]
    rows = [pltpu.VMEM((RING - 1, 8, RING, SLOTS, width), jnp.bfloat16) for width in widths]
    sums = [pltpu.VMEM((RING - 1, tokens, width), jnp.float32) for width in widths]
    dma = pltpu.SemaphoreType.DMA
    return pl.pallas_call(
        return_kernel,
        out_shape=(y, y, jax.ShapeDtypeStruct(x_b.shape, x_b.dtype)),
        in_specs=[any_spec] * 2 + [vmem_spec] * 4 + [any_spec] * 3,
        out_specs=(vmem_spec, vmem_spec, any_spec),
        scratch_shapes=back + rows + sums[:3] + sums + [pltpu.VMEM((tokens, model), jnp.float32)]
        + [dma((2, 3, RING)), dma((2, 3)), dma((2, 3)), dma((2, 3, 3)), dma((2, 3)), dma((2, 3, 3)), dma((3,))]
        + [pltpu.VMEM((3, RING, 128, 128), jnp.float32), pltpu.VMEM((4,) + x_b.shape[1:], jnp.bfloat16)]
        + expert_scratch(model, ffn),
        compiler_params=pltpu.CompilerParams(collective_id=1, has_side_effects=True, vmem_limit_bytes=63 * 1024 * 1024),
        name="return_rows",
    )(done_a, x_b, *metas, *residuals, *weights)[:2]


def hand_over_kernel(a_ref, b_ref, a_out, b_out):
    a_out[...] = a_ref[...]
    b_out[...] = b_ref[...]


def hand_over(y_a, y_b):
    return pl.pallas_call(hand_over_kernel, out_shape=tuple(jax.ShapeDtypeStruct(y.shape, y.dtype) for y in (y_a, y_b)), name="hand_over")(y_a, y_b)


def solution(mesh):
    row_spec = P(("dp", "ep"), None)
    full_spec = P(None, None, None)
    gain_spec = P(None)
    expert_spec = P("ep", None, None)
    in_specs = (row_spec,) * 8 + (gain_spec,) + (full_spec,) * 4 + (gain_spec,) + (expert_spec,) * 3

    def device_fn(tokens_a, experts_a, slots_a, gates_a, tokens_b, experts_b, slots_b, gates_b, attn_gain, w_query, w_key, w_value, w_out, moe_gain, w_gate, w_up, w_down):
        weights = (w_gate[0], w_up[0], w_down[0])
        attention_weights = [jnp.transpose(w, (1, 2, 0)) for w in (w_query, w_key, w_value)] + [w_out]
        routing = [(e.T, s.T, g.T) for e, s, g in ((experts_a, slots_a, gates_a), (experts_b, slots_b, gates_b))]
        _, x_b, meta_a, meta_b, res_a, res_b, done_a = dispatch((tokens_a, tokens_b), routing, (attn_gain, moe_gain), attention_weights, weights)
        return hand_over(*bring_back(done_a, x_b, (meta_a, meta_b), (res_a, res_b), weights))

    return jax.shard_map(device_fn, mesh=mesh, in_specs=in_specs, out_specs=(row_spec, row_spec), check_vma=False)
```

```python
import jax
import jax.numpy as jnp
from jax import lax
from jax.experimental import pallas as pl
from jax.experimental.pallas import tpu as pltpu
from jax.sharding import PartitionSpec as P

NORM_EPS = 1e-6
MASK_VALUE = -1e30
RING = 4
CORES = 2
SLOTS = 16
HEAD_DIM = 64
ORDERS = (("z", "y", "x"), ("x", "z", "y"), ("y", "x", "z"))
PARTS = (
    ((0, 640, ORDERS[0]), (640, 640, ORDERS[1]), (1280, 768, ORDERS[2])),
    ((0, 768, ORDERS[0]), (768, 640, ORDERS[1]), (1408, 640, ORDERS[2])),
)
STRIDE = {"z": 32, "y": 8, "x": 2}

def coords(index):
    return {"z": index // 32, "y": (index // 8) % RING, "x": (index // 2) % RING}, index % CORES


def peer(dim, delta, flip=0):
    me = lax.axis_index("ep")
    stride = STRIDE[dim]
    place = lax.rem(me // stride, RING)
    other = me + (lax.rem(place + delta % RING, RING) - place) * stride
    if flip:
        other = other + 1 - 2 * lax.rem(me, CORES)
    return {"ep": other}


def send(src, dst, send_sem, recv_sem, where):
    return pltpu.make_async_remote_copy(src_ref=src, dst_ref=dst, send_sem=send_sem, recv_sem=recv_sem, device_id=where, device_id_type=pl.DeviceIdType.MESH)


def drain(ref, sem):
    pltpu.make_async_copy(ref, ref, sem).wait()


def greet():
    barrier = pltpu.get_barrier_semaphore()
    count = 0
    for dim in ("x", "y", "z"):
        for delta in range(1, RING):
            for flip in range(CORES):
                pl.semaphore_signal(barrier, inc=1, device_id=peer(dim, delta, flip), device_id_type=pl.DeviceIdType.MESH)
                count += 1
    pl.semaphore_signal(barrier, inc=1, device_id=peer("x", 0, 1), device_id_type=pl.DeviceIdType.MESH)
    return barrier, count + 1


def group_view(rows, n, part, off3, flip, off2):
    start, width, (_, s2, s3) = PARTS[n][part]
    place = {s3: off3, s2: off2}
    index = tuple(place.get(dim, slice(None)) for dim in ("y", "z"))
    line = flip * RING + place["x"] if "x" in place else slice(flip * RING, (flip + 1) * RING)
    return rows.at[line, index[0], index[1], :, start : start + width]


def row_ids(order, off2):
    s1, s2, s3 = order
    pos, core = coords(lax.axis_index("ep"))
    row = lax.broadcasted_iota(jnp.int32, (128, 128), 0)
    slot, flip, off3 = row % SLOTS, (row // SLOTS) % CORES, row // (SLOTS * CORES)
    base = pos[s1] * STRIDE[s1] + lax.rem(pos[s2] + off2, RING) * STRIDE[s2] + core
    expert = base + (pos[s3] + off3) % RING * STRIDE[s3] + flip * (1 - 2 * core)
    return (expert * SLOTS + slot).astype(jnp.float32)


PAIRS = tuple((off, flip) for off in range(RING) for flip in range(CORES))


def routing_ids(meta):
    expert = meta[:, 0:128].astype(jnp.float32)
    slot = meta[:, 128:256].astype(jnp.float32)
    return jnp.where(slot >= 0, expert * SLOTS + slot, -1.0)


def rms_norm(rows_f, gain_ref):
    inv_rms = lax.rsqrt(jnp.mean(rows_f * rows_f, axis=-1, keepdims=True) + NORM_EPS)
    return rows_f * inv_rms * gain_ref[...].astype(jnp.float32).reshape(1, -1)


def attend(x_ref, gain_ref, w_refs, pool, sem, normed_t, total, last, between):
    tokens, model = x_ref.shape
    steps = w_refs[0].shape[0]

    def load(i, slot):
        for w, w_ref in enumerate(w_refs):
            pltpu.make_async_copy(w_ref.at[i], pool.at[slot * 4 + w], sem.at[slot]).start()

    if not last:
        load(0, 0)
    normed_t[...] = rms_norm(x_ref[...].astype(jnp.float32), gain_ref).T.astype(jnp.bfloat16)
    total[...] = jnp.zeros_like(total)
    seen = lax.broadcasted_iota(jnp.int32, (tokens, tokens), 0) <= lax.broadcasted_iota(jnp.int32, (tokens, tokens), 1)

    def step(i, carry):
        slot = lax.rem(i, 2)
        if last:

            @pl.when(i + 1 < steps)
            def _():
                load(i + 1, 1 - slot)

        else:
            load(lax.rem(i + 1, steps), 1 - slot)
        drain(pool.at[pl.ds(slot * 4, 4)], sem.at[slot])
        query, keys, values = (
            jnp.dot(pool[slot * 4 + w].reshape(-1, model), normed_t[...], preferred_element_type=jnp.float32).astype(jnp.bfloat16) for w in range(3)
        )
        context = []
        for start in range(0, query.shape[0], HEAD_DIM):
            head = slice(start, start + HEAD_DIM)
            scores = lax.dot_general(keys[head], query[head], (((0,), (0,)), ((), ())), preferred_element_type=jnp.float32) * (HEAD_DIM**-0.5)
            scores = jnp.where(seen, scores, MASK_VALUE)
            weight = jnp.exp(scores - jnp.max(scores, axis=0, keepdims=True))
            prob = (weight / jnp.sum(weight, axis=0, keepdims=True)).astype(jnp.bfloat16)
            context.append(jnp.dot(values[head], prob, preferred_element_type=jnp.float32).astype(jnp.bfloat16))
        context = jnp.concatenate(context, axis=0)
        total[...] += lax.dot_general(context, pool[slot * 4 + 3].reshape(-1, model), (((0,), (0,)), ((), ())), preferred_element_type=jnp.float32)
        between(i)
        return carry

    lax.fori_loop(0, steps, step, 0)


def load_weights(w_refs, held, sem):
    copies = [pltpu.make_async_copy(src, dst, sem.at[i]) for i, (src, dst) in enumerate(zip(w_refs, held))]
    for copy in copies:
        copy.start()
    return copies


def run_experts(x_ref, o_ref, held, pool, x_sem, o_sem, between):
    blocks = x_ref.shape[0]
    gate_w, up_w, down_w = held
    x_buf, o_buf = pool.at[0:2], pool.at[2:4]

    def load(b, slot):
        return pltpu.make_async_copy(x_ref.at[b], x_buf.at[slot], x_sem.at[slot])

    load(0, 0).start()

    def step(b, carry):
        slot = lax.rem(b, 2)

        @pl.when(b + 1 < blocks)
        def _():
            load(b + 1, 1 - slot).start()

        load(b, slot).wait()

        @pl.when(b >= 2)
        def _():
            drain(o_buf.at[slot], o_sem.at[slot])

        x = x_buf[slot].reshape(-1, gate_w.shape[0])
        gate_act = jnp.dot(x, gate_w[...], preferred_element_type=jnp.float32)
        up_act = jnp.dot(x, up_w[...], preferred_element_type=jnp.float32)
        hidden = (jax.nn.silu(gate_act) * up_act).astype(jnp.bfloat16)
        o_buf[slot] = jnp.dot(hidden, down_w[...], preferred_element_type=jnp.float32).astype(jnp.bfloat16).reshape(o_buf.shape[1:])
        pltpu.make_async_copy(o_buf.at[slot], o_ref.at[b], o_sem.at[slot]).start()
        between(b)
        return carry

    lax.fori_loop(0, blocks, step, 0)
    for slot in range(2):
        drain(o_buf.at[slot], o_sem.at[slot])


def expert_scratch(model, ffn):
    dma = pltpu.SemaphoreType.DMA
    return [
        pltpu.VMEM((model, ffn), jnp.bfloat16),
        pltpu.VMEM((model, ffn), jnp.bfloat16),
        pltpu.VMEM((ffn, model), jnp.bfloat16),
        dma((3,)),
        dma((2,)),
        dma((2,)),
    ]


def dispatch_kernel(*refs):
    batches = 2
    x_refs, routing_refs, gain_refs, aw_refs, w_refs = refs[0:2], (refs[2:5], refs[5:8]), refs[8:10], refs[10:14], refs[14:17]
    out_refs, meta_refs, res_refs, done_ref = refs[17:19], refs[19:21], refs[21:23], refs[23]
    scratch = refs[24:]
    planes = [scratch[3 * n : 3 + 3 * n] for n in range(batches)]
    chosen = [scratch[6 + 3 * n : 9 + 3 * n] for n in range(batches)]
    plane_recv, plane_send, row_recv, row_send, local_sem = scratch[12:17]
    own_refs, normed_t, total, ids_ref, pool, attn_sem = scratch[17:19], scratch[19], scratch[20], scratch[21], scratch[22], scratch[23]
    held, (w_sem, x_sem, o_sem) = scratch[24:27], scratch[27:]
    tokens = x_refs[0].shape[0]
    half = tokens // 2
    barrier, greetings = greet()

    def own_part(n, part):
        start, width, _ = PARTS[n][part]
        return own_refs[n].at[:, start : start + width]

    def attention(n, between):
        attend(x_refs[n], gain_refs[0], aw_refs, pool, attn_sem, normed_t, total, n == batches - 1, between)
        residual = (x_refs[n][...].astype(jnp.float32) + total[...]).astype(jnp.bfloat16)
        res_refs[n][...] = residual
        own_refs[n][0:tokens, :] = rms_norm(residual.astype(jnp.float32), gain_refs[1]).astype(jnp.bfloat16)
        own_refs[n][tokens : tokens + 8, :] = jnp.zeros((8, own_refs[n].shape[1]), jnp.bfloat16)
        for start, _, _ in PARTS[n]:
            for i, ref in enumerate(routing_refs[n]):
                own_refs[n][tokens : tokens + 8, start + i * 128 : start + (i + 1) * 128] = ref[...].astype(jnp.float32).astype(jnp.bfloat16)

    def send_own(n):
        for part, (_, _, (s1, s2, _)) in enumerate(PARTS[n]):
            plane = planes[n][part]
            for off in (1, 3):
                send(own_part(n, part), plane.at[off], plane_send.at[n, part], plane_recv.at[n, part, off], peer(s1, off)).start()
            for off in (1, 3):
                send(own_part(n, part), plane.at[off * RING], plane_send.at[n, part], plane_recv.at[n, part, off * RING], peer(s2, off)).start()

    def forward(n, far):
        for part, (_, _, (s1, s2, _)) in enumerate(PARTS[n]):
            plane = planes[n][part]
            for off1 in (2,) if far else (1, 3):
                drain(plane.at[off1], plane_recv.at[n, part, off1])
                if not far:
                    rows = slice(0, half) if off1 == 1 else slice(half, tokens + 8)
                    send(plane.at[off1, rows], plane.at[2, rows], plane_send.at[n, part], plane_recv.at[n, part, 2], peer(s1, off1)).start()
                for off2 in (1, 3):
                    send(plane.at[off1], plane.at[off2 * RING + off1], plane_send.at[n, part], plane_recv.at[n, part, off2 * RING + off1], peer(s2, off2)).start()

    def relay(n, off2):
        rows = slice(0, half) if off2 == 1 else slice(half, tokens + 8)
        for part, (_, _, (s1, s2, _)) in enumerate(PARTS[n]):
            plane = planes[n][part]
            for off1 in range(RING):
                drain(plane.at[off2 * RING + off1], plane_recv.at[n, part, off2 * RING + off1])
                send(plane.at[off2 * RING + off1, rows], plane.at[2 * RING + off1, rows], plane_send.at[n, part], plane_recv.at[n, part, 2 * RING + off1], peer(s2, off2)).start()

    def select(n, part, off2, off1, block):
        width = PARTS[n][part][1]
        ids = ids_ref[part]
        dest = routing_ids(block[tokens : tokens + 8, 0:384])
        hit = ids == dest[0:1, :]
        for j in range(1, 8):
            hit = jnp.logical_or(hit, ids == dest[j : j + 1, :])
        onehot = jnp.where(hit, 1.0, 0.0).astype(jnp.bfloat16)
        rows = jnp.dot(onehot, block[0:tokens, :], preferred_element_type=jnp.float32).astype(jnp.bfloat16)
        chosen[n][part][:, off2, off1] = rows.reshape(8, SLOTS, width)

    def select_group(n, part, off2):
        start, width, _ = PARTS[n][part]
        plane = planes[n][part]
        if off2 == 0:
            meta_refs[n][part, 0] = own_refs[n][tokens : tokens + 8, start : start + 384]
            for off1 in range(1, RING):
                meta_refs[n][part, off1] = plane[off1, tokens : tokens + 8, 0:384]
            select(n, part, 0, 0, own_refs[n].at[:, start : start + width])
            first = 1
        else:
            for off1 in range(RING if off2 == 2 else 0):
                drain(plane.at[off2 * RING + off1], plane_recv.at[n, part, off2 * RING + off1])
            first = 0

        def body(off1, carry):
            select(n, part, off2, off1, plane.at[off2 * RING + off1])
            return carry

        lax.fori_loop(first, RING, body, 0)

    def send_group(n, part, off2):
        s3 = ORDERS[part][2]
        for i in (2, 3, 6, 7, 4, 5, 1):
            off3, flip = PAIRS[i]
            send(chosen[n][part].at[i, off2], group_view(out_refs[n], n, part, off3, flip, off2), row_send.at[n, part], row_recv.at[n], peer(s3, off3, flip)).start()
        pltpu.make_async_copy(chosen[n][part].at[0, off2], group_view(out_refs[n], n, part, 0, 0, off2), local_sem.at[n, part]).start()

    late = []

    def groups(n, off2):
        for part in range(3):
            select_group(n, part, off2)
            if late:
                send_group(*late.pop())
            late.append((n, part, off2))

    def flush():
        if late:
            send_group(*late.pop())

    def under_b(i):
        @pl.when(i == 2)
        def _():
            forward(0, False)

        @pl.when(i == 6)
        def _():
            forward(0, True)

    attention(0, lambda i: None)
    pl.semaphore_wait(barrier, greetings)
    send_own(0)
    for part, order in enumerate(ORDERS):
        ids_ref[part] = row_ids(order, 0)
    attention(1, under_b)
    weight_copies = load_weights(w_refs, held, w_sem)
    send_own(1)
    groups(0, 0)
    relay(0, 1)
    relay(0, 3)
    groups(0, 1)
    forward(1, False)
    groups(0, 3)
    forward(1, True)
    flush()
    groups(0, 2)
    groups(1, 0)
    relay(1, 1)
    relay(1, 3)
    flush()
    groups(1, 1)

    def rows_done(n):
        drain(out_refs[n].at[1:8], row_recv.at[n])
        for part in range(3):
            drain(chosen[n][part].at[0], local_sem.at[n, part])

    def under_a(b):
        @pl.when(b == 1)
        def _():
            groups(1, 3)

        @pl.when(b == 4)
        def _():
            groups(1, 2)

        @pl.when(b == 5)
        def _():
            flush()

    flush()
    rows_done(0)
    for copy in weight_copies:
        copy.wait()
    run_experts(out_refs[0], done_ref, held, pool, x_sem, o_sem, under_a)
    rows_done(1)
    for n in range(batches):
        for part in range(3):
            drain(planes[n][part].at[1:16], plane_send.at[n, part])
            drain(chosen[n][part].at[1:8], row_send.at[n, part])


def dispatch(tokens, routing, gains, attention_weights, weights):
    rows, model = tokens[0].shape
    ffn = weights[0].shape[1]
    block = (RING, RING, SLOTS, model)
    out = jax.ShapeDtypeStruct((CORES * RING,) + block, jnp.bfloat16)
    meta = jax.ShapeDtypeStruct((3, RING, 8, 384), jnp.bfloat16)
    residual = jax.ShapeDtypeStruct((rows, model), jnp.bfloat16)
    any_spec, vmem_spec = pl.BlockSpec(memory_space=pl.ANY), pl.BlockSpec(memory_space=pltpu.VMEM)
    widths = [width for parts in PARTS for _, width, _ in parts]
    plane = [pltpu.VMEM((RING * RING, rows + 8, width), jnp.bfloat16) for width in widths]
    chosen = [pltpu.VMEM((8, RING, RING, SLOTS, width), jnp.bfloat16) for width in widths]
    own = pltpu.VMEM((rows + 8, model), jnp.bfloat16)
    dma = pltpu.SemaphoreType.DMA
    return pl.pallas_call(
        dispatch_kernel,
        out_shape=(out, out, meta, meta, residual, residual, out),
        in_specs=[vmem_spec] * 10 + [any_spec] * 7,
        out_specs=(any_spec,) * 2 + (vmem_spec,) * 4 + (any_spec,),
        scratch_shapes=plane
        + chosen
        + [dma((2, 3, 16)), dma((2, 3)), dma((2,)), dma((2, 3)), dma((2, 3))]
        + [own, own, pltpu.VMEM((model, rows), jnp.bfloat16), pltpu.VMEM((rows, model), jnp.float32), pltpu.VMEM((3, 128, 128), jnp.float32)]
        + [pltpu.VMEM((8,) + block, jnp.bfloat16), dma((2,))]
        + expert_scratch(model, ffn),
        compiler_params=pltpu.CompilerParams(collective_id=0, has_side_effects=True, vmem_limit_bytes=63 * 1024 * 1024),
        name="dispatch_rows",
    )(*tokens, *routing[0], *routing[1], *gains, *(w.reshape((8,) + block) for w in attention_weights), *weights)


def return_kernel(*refs):
    batches = 2
    done_a, x_b, meta_refs, res_refs, w_refs = refs[0], refs[1], refs[2:4], refs[4:6], refs[6:9]
    y_refs, done_b, scratch = refs[9:11], refs[11], refs[12:]
    out_refs = (done_a, done_b)
    back = [scratch[0 + 3 * n : 3 + 3 * n] for n in range(batches)]
    rows = [scratch[6 + 3 * n : 9 + 3 * n] for n in range(batches)]
    sums = (scratch[12:15], scratch[12:15][::-1])
    got = [scratch[15 + 3 * n : 18 + 3 * n] for n in range(batches)]
    kept = scratch[21]
    back_recv, back_send, own_sem, rows_recv, rows_send, sums_recv, sums_send = scratch[22:29]
    ids_ref, pool = scratch[29:31]
    held, (w_sem, x_sem, o_sem) = scratch[31:34], scratch[34:]
    tokens = y_refs[0].shape[0]
    barrier, greetings = greet()
    for part, order in enumerate(ORDERS):
        for off2 in range(RING):
            ids_ref[part, off2] = row_ids(order, off2)
    pl.semaphore_wait(barrier, greetings)
    weight_copies = load_weights(w_refs, held, w_sem)

    def hand_out(n):
        for part in range(3):
            for off2 in range(RING):
                pltpu.make_async_copy(group_view(out_refs[n], n, part, 0, 0, off2), back[n][part].at[0, off2], own_sem.at[n, part]).start()
        for off2 in (2, 1, 3, 0):
            for i in (2, 3, 6, 7, 4, 5, 1):
                off3, flip = PAIRS[i]
                for part in range(3):
                    s3 = ORDERS[part][2]
                    send(group_view(out_refs[n], n, part, off3, flip, off2), back[n][part].at[i, off2], back_send.at[n, part], back_recv.at[n, part, off2], peer(s3, -off3, flip)).start()

    def turn(n, off2):
        for part in range(3):
            s2 = ORDERS[part][1]
            drain(back[n][part].at[1:8, off2], back_recv.at[n, part, off2])
            if off2:
                send(back[n][part].at[:, off2], rows[n][part].at[off2 - 1], rows_send.at[n, part], rows_recv.at[n, part, off2 - 1], peer(s2, -off2)).start()

    def weighted(n, part, off2, off1):
        width = PARTS[n][part][1]
        meta = meta_refs[n][part, off1]
        dest = routing_ids(meta)
        gates = meta[:, 256:384].astype(jnp.float32)
        ids = ids_ref[part, off2]
        weight = jnp.zeros((128, tokens), jnp.float32)
        for j in range(8):
            weight = jnp.where(ids == dest[j : j + 1, :], gates[j : j + 1, :], weight)
        block = back[n][part][:, 0, off1] if off2 == 0 else rows[n][part][off2 - 1, :, off1]
        return lax.dot_general(weight.astype(jnp.bfloat16), block.reshape(128, width), (((0,), (0,)), ((), ())), preferred_element_type=jnp.float32)

    def own_ready(n):
        for part in range(3):
            drain(back[n][part].at[0], own_sem.at[n, part])

    def add_group(n, off2, first=False, last=False):
        late = []

        def flush():
            if late:
                part = late.pop()
                s1 = ORDERS[part][0]
                for rows_half, off in ((slice(0, tokens // 2), -1), (slice(tokens // 2, tokens), 1)):
                    send(sums[n][part].at[1, rows_half], got[n][part].at[2, rows_half], sums_send.at[part], sums_recv.at[n, part, 2], peer(s1, off)).start()

        for part in range(3):
            start, width, _ = PARTS[n][part]
            if off2:
                drain(rows[n][part].at[off2 - 1], rows_recv.at[n, part, off2 - 1])
            for off1 in (2, 1, 3, 0):
                term = weighted(n, part, off2, off1)
                if off1 == 0:
                    before = res_refs[n][:, start : start + width].astype(jnp.float32) if first else kept[:, start : start + width]
                    kept[:, start : start + width] = before + term
                else:
                    sums[n][part][off1 - 1] = term if first else sums[n][part][off1 - 1] + term
                flush()
                if last and off1 == 2:
                    late.append(part)

    def pass_on(n):
        def out(part):
            s1 = ORDERS[part][0]
            for off1, place in ((1, 0), (3, 1)):
                send(sums[n][part].at[off1 - 1], got[n][part].at[place], sums_send.at[part], sums_recv.at[n, part, place], peer(s1, -off1)).start()

        middle = tokens // 2
        for part in range(3):
            drain(got[n][part].at[2], sums_recv.at[n, part, 2])
            sums[n][part][0, 0:middle] = sums[n][part][0, 0:middle] + got[n][part][2, 0:middle]
            sums[n][part][2, middle:] = sums[n][part][2, middle:] + got[n][part][2, middle:]
            if part:
                out(part - 1)
        out(2)

    def finish(n):
        for part in range(3):
            start, width, _ = PARTS[n][part]
            total = kept[:, start : start + width]
            for place in range(2):
                drain(got[n][part].at[place], sums_recv.at[n, part, place])
                total = total + got[n][part][place]
            y_refs[n][:, start : start + width] = total.astype(y_refs[n].dtype)
            drain(sums[n][part], sums_send.at[part])

    hand_out(0)
    for copy in weight_copies:
        copy.wait()

    def between(b):
        for when, off2 in ((2, 2), (4, 1), (6, 3)):

            @pl.when(b == when)
            def _():
                if off2 == 2:
                    own_ready(0)
                turn(0, off2)

    run_experts(x_b, done_b, held, pool, x_sem, o_sem, between)
    hand_out(1)
    turn(0, 0)
    add_group(0, 0, first=True)
    add_group(0, 2)
    add_group(0, 1)
    own_ready(1)
    turn(1, 2)
    add_group(0, 3, last=True)
    turn(1, 1)
    pass_on(0)
    turn(1, 3)
    turn(1, 0)
    finish(0)
    add_group(1, 0, first=True)
    add_group(1, 2)
    add_group(1, 1)
    add_group(1, 3, last=True)
    pass_on(1)
    finish(1)
    for n in range(batches):
        for part in range(3):
            drain(back[n][part].at[1:8], back_send.at[n, part])
            drain(rows[n][part], rows_send.at[n, part])


def bring_back(done_a, x_b, metas, residuals, weights):
    tokens, model = residuals[0].shape
    ffn = weights[0].shape[1]
    y = jax.ShapeDtypeStruct((tokens, model), jnp.bfloat16)
    any_spec, vmem_spec = pl.BlockSpec(memory_space=pl.ANY), pl.BlockSpec(memory_space=pltpu.VMEM)
    widths = [width for parts in PARTS for _, width, _ in parts]
    back = [pltpu.VMEM((8, RING, RING, SLOTS, width), jnp.bfloat16) for width in widths]
    rows = [pltpu.VMEM((RING - 1, 8, RING, SLOTS, width), jnp.bfloat16) for width in widths]
    sums = [pltpu.VMEM((RING - 1, tokens, width), jnp.float32) for width in widths]
    dma = pltpu.SemaphoreType.DMA
    return pl.pallas_call(
        return_kernel,
        out_shape=(y, y, jax.ShapeDtypeStruct(x_b.shape, x_b.dtype)),
        in_specs=[any_spec] * 2 + [vmem_spec] * 4 + [any_spec] * 3,
        out_specs=(vmem_spec, vmem_spec, any_spec),
        scratch_shapes=back + rows + sums[:3] + sums + [pltpu.VMEM((tokens, model), jnp.float32)]
        + [dma((2, 3, RING)), dma((2, 3)), dma((2, 3)), dma((2, 3, 3)), dma((2, 3)), dma((2, 3, 3)), dma((3,))]
        + [pltpu.VMEM((3, RING, 128, 128), jnp.float32), pltpu.VMEM((4,) + x_b.shape[1:], jnp.bfloat16)]
        + expert_scratch(model, ffn),
        compiler_params=pltpu.CompilerParams(collective_id=1, has_side_effects=True, vmem_limit_bytes=63 * 1024 * 1024),
        name="return_rows",
    )(done_a, x_b, *metas, *residuals, *weights)[:2]


def hand_over_kernel(a_ref, b_ref, a_out, b_out):
    a_out[...] = a_ref[...]
    b_out[...] = b_ref[...]


def hand_over(y_a, y_b):
    return pl.pallas_call(hand_over_kernel, out_shape=tuple(jax.ShapeDtypeStruct(y.shape, y.dtype) for y in (y_a, y_b)), name="hand_over")(y_a, y_b)


def solution(mesh):
    row_spec = P(("dp", "ep"), None)
    full_spec = P(None, None, None)
    gain_spec = P(None)
    expert_spec = P("ep", None, None)
    in_specs = (row_spec,) * 8 + (gain_spec,) + (full_spec,) * 4 + (gain_spec,) + (expert_spec,) * 3

    def device_fn(tokens_a, experts_a, slots_a, gates_a, tokens_b, experts_b, slots_b, gates_b, attn_gain, w_query, w_key, w_value, w_out, moe_gain, w_gate, w_up, w_down):
        weights = (w_gate[0], w_up[0], w_down[0])
        attention_weights = [jnp.transpose(w, (1, 2, 0)) for w in (w_query, w_key, w_value)] + [w_out]
        routing = [(e.T, s.T, g.T) for e, s, g in ((experts_a, slots_a, gates_a), (experts_b, slots_b, gates_b))]
        _, x_b, meta_a, meta_b, res_a, res_b, done_a = dispatch((tokens_a, tokens_b), routing, (attn_gain, moe_gain), attention_weights, weights)
        return hand_over(*bring_back(done_a, x_b, (meta_a, meta_b), (res_a, res_b), weights))

    return jax.shard_map(device_fn, mesh=mesh, in_specs=in_specs, out_specs=(row_spec, row_spec), check_vma=False)
```
